512 devices in a mesh: rep: 4 (over x_hi, core), row: 32 (over x_lo, z), col: 4 (over y).
Axes of the slice: x: 4 (x_hi: 2, x_lo: 2; x = x_hi * 2 + x_lo), y: 4, z: 16, core: 2. Of those that a mesh axis runs over, the one named last changes fastest.
Arguments:
- spin_init: bfloat16 [256, 8192], P('rep', 'row'), may hold values from -1 to 1, as said below
- couplings: bfloat16 [32, 4, 64, 8192], P(None, 'col', None, 'row'), may hold values from -1 to 1, as said below
- flip_noise: float32 [10, 256, 8192], P(None, 'rep', 'row'), may hold values from 0 to 17, as said below
- colors: int32 [8192], P('row'), may hold values 0 or 1
- beta_steps: int32 [256], replicated, may hold values from 96 to 1024
- partners: int32 [256], replicated, may hold values from 0 to 255, as said below
- swap_noise: float32 [256], replicated, may hold values from 0 to 17, as said below
Outputs:
- spins_out: bfloat16 [256, 8192], P('rep', 'row')
- energies: float32 [256], P('rep')
The draws below stay inside these ranges and needn't reach their ends.
Inputs may be any that keep to these rules, and one draw needn't show every extreme that they name: `spin_init`: every entry is -1 or +1. `couplings`: the 8192 x 8192 matrix is symmetric, zero on its diagonal, and every other entry is -1 or +1. `flip_noise`: independent exponential variates of mean one. `swap_noise`: independent exponential variates of mean one. Pairs slots: partners[partners[r]] = r and partners[r] != r for every slot.
All inputs are finite; a program needn't handle non-finite values. No bound on the sum of `colors` on one device may be relied on, other than what follows from the above.
Results may differ from the reference program's by a relative error of at most 0.001.
Values may be sent and summed in bfloat16 or wider, within the bound.
No kernel may reach another device: no remote copies, remote signals or barrier semaphores. Data moves between devices by JAX's collectives and lax.ppermute only.
A program may use at most 64 MiB of HBM per device.

```python
import math
import jax
import jax.numpy as jnp
from jax import lax

N = 8192
SWEEPS = 10
R = 256
PIECE = 64
N_ROW = 32
N_COL = 4


def draw_spin_init(key, part):
    coin_flips = jax.random.randint(key, (R, N), 0, 2)
    return (coin_flips.astype(jnp.float32) * 2.0 - 1.0).astype(jnp.bfloat16)


def draw_couplings(key, part):
    coin_flips = jax.random.randint(key, (N, N), 0, 2).astype(jnp.float32) * 2.0 - 1.0
    row_ids = jnp.arange(N)[:, None]
    col_ids = jnp.arange(N)[None, :]
    symmetric = jnp.where(row_ids < col_ids, coin_flips, coin_flips.T)
    symmetric = jnp.where(row_ids == col_ids, 0.0, symmetric)
    return symmetric.astype(jnp.float32).reshape(N_ROW, N_COL, PIECE, N).astype(jnp.bfloat16)


def draw_flip_noise(key, part):
    return jax.random.exponential(key, (SWEEPS, R, N), jnp.float32)


def draw_swap_noise(key, part):
    return jax.random.exponential(key, (R,), jnp.float32)


def draw_partners(key, part):
    shuffled = jax.random.permutation(key, R).astype(jnp.int32)
    first_half = shuffled[0::2]
    second_half = shuffled[1::2]
    mate_table = jnp.zeros((R,), jnp.int32)
    mate_table = mate_table.at[first_half].set(second_half)
    mate_table = mate_table.at[second_half].set(first_half)
    return mate_table


def set_ends(drawn, rng, least, largest):
    place = [jax.random.randint(jax.random.fold_in(rng, axis), (), 0, length) for axis, length in enumerate(drawn.shape)]
    widest = drawn.shape.index(max(drawn.shape))
    neighbour = place[:widest] + [(place[widest] + 1) % drawn.shape[widest]] + place[widest + 1:]
    return drawn.at[tuple(place)].set(least).at[tuple(neighbour)].set(largest)


def setup_inputs(seed: int = 0) -> dict:
    seeds = jax.random.split(jax.random.key(seed), 8)
    return {
        "spin_init": draw_spin_init(jax.random.fold_in(seeds[7], 71), 0),
        "couplings": draw_couplings(jax.random.fold_in(seeds[7], 71), 0),
        "flip_noise": draw_flip_noise(jax.random.fold_in(seeds[7], 71), 0),
        "colors": set_ends((jax.random.randint(seeds[3], (N,), 0, 2) < 1).astype(jnp.int32), jax.random.fold_in(seeds[3], 1), 0, 1),
        "beta_steps": set_ends(jax.random.randint(seeds[4], (R,), 96, 1025), jax.random.fold_in(seeds[4], 1), 96, 1024).astype(jnp.int32),
        "partners": draw_partners(jax.random.fold_in(seeds[7], 71), 0),
        "swap_noise": draw_swap_noise(jax.random.fold_in(seeds[7], 71), 0),
    }


def reference(spin_init, couplings, flip_noise, colors, beta_steps, partners, swap_noise):
    matrix = couplings.reshape(N, N).astype(jnp.float32)
    spin_state = spin_init.astype(jnp.float32)
    beta_col = beta_steps.astype(jnp.float32)[:, None]
    for step_index in range(SWEEPS):
        fields = jnp.dot(spin_state, matrix, precision=lax.Precision.HIGHEST, preferred_element_type=jnp.float32)
        energy_cost = beta_col * (spin_state * fields) * (1.0 / 16384.0)
        flipped = (colors == step_index % 2)[None, :] & (energy_cost < flip_noise[step_index])
        spin_state = jnp.where(flipped, -spin_state, spin_state)
    fields = jnp.dot(spin_state, matrix, precision=lax.Precision.HIGHEST, preferred_element_type=jnp.float32)
    energy = -0.5 * lax.optimization_barrier(jnp.sum(spin_state * fields, axis=1))
    slot_ids = jnp.arange(R, dtype=jnp.int32)
    all_betas = beta_steps.astype(jnp.float32)
    mate_energy = energy[partners]
    swap_gain = (all_betas - all_betas[partners]) * (energy - mate_energy) * (1.0 / (64.0 * N * math.sqrt(N)))
    accept = swap_gain + swap_noise[jnp.minimum(slot_ids, partners)] > 0.0
    spins_out = jnp.where(accept[:, None], spin_state[partners], spin_state).astype(jnp.bfloat16)
    energies = jnp.where(accept, mate_energy, energy) * (1.0 / (N * math.sqrt(N)))
    return (spins_out, energies)
```

```python
import math

import jax
import jax.numpy as jnp
from jax import lax
from jax.sharding import Mesh, PartitionSpec as P

N = 8192
SWEEPS = 10
NEVER = -3.0e38

GROUP = ("xh", "core")
PLANE = ("xl", "y")
LAYER = ("xh", "core", "xl", "y")


def sent_to_all(value, axes):
    length = lax.axis_size(axes)
    return lax.all_to_all(
        jnp.broadcast_to(value[None], (length, *value.shape)), axes, 0, 0, tiled=True
    )


def per_device(spin_init, couplings, flip_noise, colors, beta_steps, partners, swap_noise):
    rep_dev, row_width = spin_init.shape
    n_xl = lax.axis_size("xl")
    n_y = lax.axis_size("y")
    n_z = lax.axis_size("z")
    n_core = lax.axis_size("core")
    y_index = lax.axis_index("y")
    core_index = lax.axis_index("core")
    rep_index = lax.axis_index(GROUP)
    share = rep_dev // (n_xl * n_y)
    piece = row_width // n_y
    width = n_xl * row_width
    own_block = couplings.reshape(-1, row_width)

    core_part = lax.dynamic_slice_in_dim(
        couplings.reshape(n_core, -1, row_width), core_index, 1, 0
    )[0]
    gathered = lax.all_gather(core_part, ("core", *PLANE))
    layer_block = (
        gathered.reshape(n_core, n_xl, n_y, n_z, piece, row_width)
        .transpose(3, 0, 2, 4, 1, 5)
        .reshape(N, width)
    )

    start_piece = lax.dynamic_slice_in_dim(spin_init, y_index * piece, piece, 1)
    start_rows = sent_to_all(start_piece, ("xl", "z"))
    start_rows = start_rows.transpose(1, 0, 2).reshape(rep_dev, -1)
    partial = jnp.dot(start_rows, own_block, preferred_element_type=jnp.float32)
    partial = lax.all_to_all(
        partial.reshape(n_xl * n_y, share, row_width), PLANE, 0, 0, tiled=True
    )
    fields = partial.reshape(n_xl, n_y, share, row_width).sum(axis=1)
    fields = fields.transpose(1, 0, 2).reshape(share, width)

    steps = jnp.arange(SWEEPS, dtype=jnp.int32)[:, None, None]
    limits = jnp.where(colors[None, None, :] == steps % 2, flip_noise, NEVER)
    both = jnp.concatenate([spin_init.astype(jnp.float32)[None], limits], axis=0)
    both = both.reshape(SWEEPS + 1, n_xl, n_y, share, row_width)
    both = lax.dynamic_index_in_dim(both, y_index, 2, keepdims=False)
    both = lax.all_to_all(both.transpose(1, 0, 2, 3), "xl", 0, 0, tiled=True)
    both = both.transpose(1, 2, 0, 3).reshape(SWEEPS + 1, share, width)
    spins = both[0]
    limits = both[1:]
    first_slot = rep_index * rep_dev + lax.axis_index(PLANE) * share
    beta_col = lax.dynamic_slice_in_dim(beta_steps, first_slot, share).astype(jnp.float32)
    beta_col = beta_col[:, None] * (1.0 / 16384.0)

    def metropolis(spins, fields, limit):
        energy_cost = beta_col * (spins * fields)
        return jnp.where(energy_cost < limit, -spins, spins)

    def layer_fields(spins):
        rows = sent_to_all(spins.astype(jnp.bfloat16), "z")
        rows = rows.transpose(1, 0, 2).reshape(share, N)
        return jnp.dot(rows, layer_block, preferred_element_type=jnp.float32)

    spins = metropolis(spins, fields, limits[0])
    for step in range(1, SWEEPS):
        spins = metropolis(spins, layer_fields(spins), limits[step])

    blocks = spins.astype(jnp.bfloat16).reshape(share, n_xl, row_width).transpose(1, 0, 2)
    blocks = jnp.broadcast_to(
        blocks[None, :, None], (lax.axis_size(GROUP), n_xl, n_y, share, row_width)
    ).reshape(-1, share, row_width)
    every_spins = lax.all_to_all(blocks, LAYER, 0, 0, tiled=True).reshape(-1, row_width)

    layer_sum = jnp.sum(spins * layer_fields(spins), axis=1)
    layer_sum = jnp.pad(layer_sum[None], ((0, 0), (0, 128 - share)))
    energy = -0.5 * sent_to_all(layer_sum, "z").sum(axis=0)
    every_energy = sent_to_all(energy, LAYER)[:, 0, :share].reshape(-1)

    slot_ids = rep_index * rep_dev + jnp.arange(rep_dev, dtype=jnp.int32)
    mate_ids = lax.dynamic_slice_in_dim(partners, rep_index * rep_dev, rep_dev)
    all_ids = jnp.arange(every_energy.shape[0], dtype=jnp.int32)[None, :]

    def picked(table, ids):
        return jnp.sum(jnp.where(ids[:, None] == all_ids, table[None, :], 0.0), axis=1)

    all_betas = beta_steps.astype(jnp.float32)
    own_energy = picked(every_energy, slot_ids)
    mate_energy = picked(every_energy, mate_ids)
    swap_gain = (
        (picked(all_betas, slot_ids) - picked(all_betas, mate_ids))
        * (own_energy - mate_energy)
        * (1.0 / (64.0 * N * math.sqrt(N)))
    )
    accept = swap_gain + picked(swap_noise, jnp.minimum(slot_ids, mate_ids)) > 0.0
    source = jnp.where(accept, mate_ids, slot_ids)
    chosen = (source[:, None] == all_ids).astype(jnp.bfloat16)
    spins_out = jnp.dot(chosen, every_spins, preferred_element_type=jnp.float32)
    energies = jnp.where(accept, mate_energy, own_energy) * (1.0 / (N * math.sqrt(N)))
    return (spins_out.astype(jnp.bfloat16), energies)


def solution(mesh):
    fine = Mesh(mesh.devices.reshape(2, 2, 2, 16, 4), ("xh", "core", "xl", "z", "y"))
    rep, row, col = ("xh", "core"), ("xl", "z"), "y"
    in_specs = (
        P(rep, row),
        P(None, col, None, row),
        P(None, rep, row),
        P(row),
        P(),
        P(),
        P(),
    )
    out_specs = (P(rep, row), P(rep))
    return jax.shard_map(
        per_device, mesh=fine, in_specs=in_specs, out_specs=out_specs, check_vma=False
    )
```

```python
import math

import jax
import jax.numpy as jnp
from jax import lax
from jax.experimental import pallas as pl
from jax.experimental.pallas import tpu as pltpu
from jax.sharding import Mesh, PartitionSpec as P

N = 8192
SWEEPS = 10
NEVER = -3.0e38

GROUP = ("xh", "core")
PLANE = ("xl", "y")
LAYER = ("xh", "core", "xl", "y")


def sent_to_all(value, axes):
    length = lax.axis_size(axes)
    return lax.all_to_all(
        jnp.broadcast_to(value[None], (length, *value.shape)), axes, 0, 0, tiled=True
    )


def in_spin_order(gathered):
    n_core, n_xl, n_y, n_z, piece, width = gathered.shape
    shape = (n_z, n_core * n_y, piece, width)

    def body(source, *rest):
        halves, sems = rest[:n_xl], rest[n_xl]
        copies = [
            pltpu.make_async_copy(
                source.at[core, xl, y],
                halves[xl].at[:, core * n_y + y],
                sems.at[core, xl, y],
            )
            for xl in range(n_xl)
            for core in range(n_core)
            for y in range(n_y)
        ]
        for copy in copies:
            copy.start()
        for copy in copies:
            copy.wait()

    halves = pl.pallas_call(
        body,
        in_specs=[pl.BlockSpec(memory_space=pltpu.HBM)],
        out_specs=[pl.BlockSpec(memory_space=pl.ANY)] * n_xl,
        out_shape=[jax.ShapeDtypeStruct(shape, gathered.dtype)] * n_xl,
        scratch_shapes=[pltpu.SemaphoreType.DMA((n_core, n_xl, n_y))],
        compiler_params=pltpu.CompilerParams(vmem_limit_bytes=2 * 1024 * 1024),
        name="in_spin_order",
    )(pltpu.with_memory_space_constraint(gathered, pltpu.HBM))
    return [half.reshape(-1, width) for half in halves]


def per_device(spin_init, couplings, flip_noise, colors, beta_steps, partners, swap_noise):
    rep_dev, row_width = spin_init.shape
    n_xl = lax.axis_size("xl")
    n_y = lax.axis_size("y")
    n_z = lax.axis_size("z")
    n_core = lax.axis_size("core")
    y_index = lax.axis_index("y")
    xl_index = lax.axis_index("xl")
    core_index = lax.axis_index("core")
    rep_index = lax.axis_index(GROUP)
    share = rep_dev // (n_xl * n_y)
    piece = row_width // n_y
    width = n_xl * row_width
    own_block = couplings.reshape(-1, row_width)

    core_part = lax.dynamic_slice_in_dim(
        couplings.reshape(n_core, -1, row_width), core_index, 1, 0
    )[0]
    gathered = lax.all_gather(core_part, ("core", *PLANE))

    start_piece = lax.dynamic_slice_in_dim(spin_init, y_index * piece, piece, 1)
    start_rows = sent_to_all(start_piece, ("xl", "z"))

    slot_ids = rep_index * rep_dev + jnp.arange(rep_dev, dtype=jnp.int32)
    mate_ids = lax.dynamic_slice_in_dim(partners, rep_index * rep_dev, rep_dev)
    all_ids = jnp.arange(partners.shape[0], dtype=jnp.int32)[None, :]

    def picked(values, ids):
        return jnp.sum(jnp.where(ids[:, None] == all_ids, values[None, :], 0.0), axis=1)

    all_betas = beta_steps.astype(jnp.float32)
    beta_gap = picked(all_betas, slot_ids) - picked(all_betas, mate_ids)
    noise = picked(swap_noise, jnp.minimum(slot_ids, mate_ids))
    mate_rows_of = (mate_ids[:, None] == all_ids).astype(jnp.bfloat16)
    start_rows, beta_gap, noise, mate_rows_of = lax.optimization_barrier(
        (start_rows, beta_gap, noise, mate_rows_of)
    )
    start_rows = start_rows.transpose(1, 0, 2).reshape(rep_dev, -1)
    partial = jnp.dot(start_rows, own_block, preferred_element_type=jnp.float32)
    partial = lax.all_to_all(
        partial.reshape(n_xl * n_y, share, row_width), PLANE, 0, 0, tiled=True
    )
    fields = partial.reshape(n_xl, n_y, share, row_width).sum(axis=1)
    fields = fields.transpose(1, 0, 2).reshape(share, width)

    steps = jnp.arange(SWEEPS, dtype=jnp.int32)[:, None, None]

    def start_of(xl):
        first = (xl * n_y + y_index) * share
        noise = lax.dynamic_slice_in_dim(flip_noise, first, share, 1)
        limits = jnp.where(colors[None, None, :] == steps % 2, noise, NEVER)
        spins = lax.dynamic_slice_in_dim(spin_init, first, share, 0)
        return jnp.concatenate([spins.astype(jnp.float32)[None], limits], axis=0)

    kept = start_of(xl_index)
    other = lax.ppermute(start_of(1 - xl_index), "xl", [(0, 1), (1, 0)])
    is_left = xl_index == 0
    both = jnp.concatenate(
        [jnp.where(is_left, kept, other), jnp.where(is_left, other, kept)], axis=2
    )
    spins = both[0]
    limits = both[1:]
    first_slot = rep_index * rep_dev + lax.axis_index(PLANE) * share
    beta_col = lax.dynamic_slice_in_dim(beta_steps, first_slot, share).astype(jnp.float32)
    beta_col = beta_col[:, None] * (1.0 / 16384.0)

    def metropolis(spins, fields, limit):
        energy_cost = beta_col * (spins * fields)
        return jnp.where(energy_cost < limit, -spins, spins)

    def layer_rows(spins):
        return sent_to_all(spins.astype(jnp.bfloat16), "z")

    def layer_fields(rows, layer_block):
        rows = rows.transpose(1, 0, 2).reshape(share, N)
        halves = [jnp.dot(rows, half, preferred_element_type=jnp.float32) for half in layer_block]
        return jnp.concatenate(halves, axis=1)

    spins = metropolis(spins, fields, limits[0])
    rows, gathered = lax.optimization_barrier((layer_rows(spins), gathered))
    layer_block = in_spin_order(
        gathered.reshape(n_core, n_xl, n_y, n_z, piece, row_width)
    )
    for step in range(1, SWEEPS):
        spins = metropolis(spins, layer_fields(rows, layer_block), limits[step])
        rows = layer_rows(spins)

    layer_sum = jnp.sum(spins * layer_fields(rows, layer_block), axis=1, keepdims=True)
    layer_sum = jnp.broadcast_to(layer_sum, (share, 128))
    energy = -0.5 * sent_to_all(layer_sum, "z").sum(axis=0)

    high = lax.reduce_precision(energy, 8, 7)
    middle = lax.reduce_precision(energy - high, 8, 7)
    low = (energy - high) - middle
    terms = jnp.concatenate(
        [high[:, :1], middle[:, :1], low[:, :1], jnp.zeros((share, 125), jnp.float32)], axis=1
    )
    blocks = spins.astype(jnp.bfloat16).reshape(share, n_xl, row_width).transpose(1, 0, 2)
    terms = jnp.broadcast_to(terms.astype(jnp.bfloat16)[None], (n_xl, share, 128))
    blocks = jnp.concatenate([blocks, terms], axis=2)
    blocks = jnp.broadcast_to(
        blocks[None, :, None], (lax.axis_size(GROUP), n_xl, n_y, *blocks.shape[1:])
    ).reshape(-1, *blocks.shape[1:])
    table = lax.all_to_all(blocks, LAYER, 0, 0, tiled=True).reshape(-1, row_width + 128)

    own_rows = lax.dynamic_slice_in_dim(table, rep_index * rep_dev, rep_dev, 0)
    own_rows = own_rows.astype(jnp.float32)
    mate_rows = jnp.dot(mate_rows_of, table, preferred_element_type=jnp.float32)

    def energy_of(rows):
        return rows[:, row_width] + (rows[:, row_width + 1] + rows[:, row_width + 2])

    own_energy = energy_of(own_rows)
    mate_energy = energy_of(mate_rows)
    swap_gain = beta_gap * (own_energy - mate_energy) * (1.0 / (64.0 * N * math.sqrt(N)))
    accept = swap_gain + noise > 0.0
    spins_out = jnp.where(
        accept[:, None], mate_rows[:, :row_width], own_rows[:, :row_width]
    )
    energies = jnp.where(accept, mate_energy, own_energy) * (1.0 / (N * math.sqrt(N)))
    return (spins_out.astype(jnp.bfloat16), energies)


def solution(mesh):
    fine = Mesh(mesh.devices.reshape(2, 2, 2, 16, 4), ("xh", "core", "xl", "z", "y"))
    rep, row, col = ("xh", "core"), ("xl", "z"), "y"
    in_specs = (
        P(rep, row),
        P(None, col, None, row),
        P(None, rep, row),
        P(row),
        P(),
        P(),
        P(),
    )
    out_specs = (P(rep, row), P(rep))
    return jax.shard_map(
        per_device, mesh=fine, in_specs=in_specs, out_specs=out_specs, check_vma=False
    )
```

```python
import math

import jax
import jax.numpy as jnp
from jax import lax
from jax.experimental import pallas as pl
from jax.experimental.pallas import tpu as pltpu
from jax.sharding import Mesh, PartitionSpec as P

N = 8192
SWEEPS = 10
NEVER = -3.0e38

GROUP = ("xh", "core")
PLANE = ("xl", "y")
LAYER = ("xh", "core", "xl", "y")


def sent_to_all(value, axes):
    length = lax.axis_size(axes)
    return lax.all_to_all(
        jnp.broadcast_to(value[None], (length, *value.shape)), axes, 0, 0, tiled=True
    )


def in_spin_order(gathered):
    n_core, n_xl, n_y, n_z, piece, width = gathered.shape
    shape = (n_z, n_core * n_y, piece, width)

    def body(source, *rest):
        halves, sems = rest[:n_xl], rest[n_xl]
        copies = [
            pltpu.make_async_copy(
                source.at[core, xl, y],
                halves[xl].at[:, core * n_y + y],
                sems.at[core, xl, y],
            )
            for xl in range(n_xl)
            for core in range(n_core)
            for y in range(n_y)
        ]
        for copy in copies:
            copy.start()
        for copy in copies:
            copy.wait()

    halves = pl.pallas_call(
        body,
        in_specs=[pl.BlockSpec(memory_space=pltpu.HBM)],
        out_specs=[pl.BlockSpec(memory_space=pl.ANY)] * n_xl,
        out_shape=[jax.ShapeDtypeStruct(shape, gathered.dtype)] * n_xl,
        scratch_shapes=[pltpu.SemaphoreType.DMA((n_core, n_xl, n_y))],
        compiler_params=pltpu.CompilerParams(vmem_limit_bytes=2 * 1024 * 1024),
        name="in_spin_order",
    )(pltpu.with_memory_space_constraint(gathered, pltpu.HBM))
    return [half.reshape(-1, width) for half in halves]


def per_device(spin_init, couplings, flip_noise, colors, beta_steps, partners, swap_noise):
    rep_dev, row_width = spin_init.shape
    n_xl = lax.axis_size("xl")
    n_y = lax.axis_size("y")
    n_z = lax.axis_size("z")
    n_core = lax.axis_size("core")
    y_index = lax.axis_index("y")
    xl_index = lax.axis_index("xl")
    core_index = lax.axis_index("core")
    rep_index = lax.axis_index(GROUP)
    share = rep_dev // (n_xl * n_y)
    piece = row_width // n_y
    width = n_xl * row_width
    own_block = couplings.reshape(-1, row_width)

    core_part = lax.dynamic_slice_in_dim(
        couplings.reshape(n_core, -1, row_width), core_index, 1, 0
    )[0]
    gathered = lax.all_gather(core_part, ("core", *PLANE))

    first_slot = rep_index * rep_dev
    all_betas = beta_steps.astype(jnp.float32)
    all_scales = all_betas * (1.0 / 16384.0)

    def metropolis(spins, fields, limit, first):
        scale = lax.dynamic_slice_in_dim(all_scales, first, spins.shape[0])[:, None]
        energy_cost = scale * (spins * fields)
        return jnp.where(energy_cost < limit, -spins, spins)

    terms = lax.dot_general(
        spin_init, own_block, (((1,), (1,)), ((), ())), preferred_element_type=jnp.float32
    )
    terms = terms.astype(jnp.bfloat16).reshape(rep_dev, -1, piece).transpose(1, 0, 2)
    terms = lax.all_to_all(terms, ("xl", "z"), 0, 0, tiled=True)

    slot_ids = first_slot + jnp.arange(rep_dev, dtype=jnp.int32)
    mate_ids = lax.dynamic_slice_in_dim(partners, first_slot, rep_dev)
    all_ids = jnp.arange(partners.shape[0], dtype=jnp.int32)[None, :]

    def picked(values, ids):
        return jnp.sum(jnp.where(ids[:, None] == all_ids, values[None, :], 0.0), axis=1)

    beta_gap = picked(all_betas, slot_ids) - picked(all_betas, mate_ids)
    noise = picked(swap_noise, jnp.minimum(slot_ids, mate_ids))
    mate_rows_of = (mate_ids[:, None] == all_ids).astype(jnp.bfloat16)
    terms, beta_gap, noise, mate_rows_of = lax.optimization_barrier(
        (terms, beta_gap, noise, mate_rows_of)
    )

    def own_piece(value):
        return lax.dynamic_slice_in_dim(value, y_index * piece, piece, value.ndim - 1)

    limit = jnp.where(own_piece(colors)[None, :] == 0, own_piece(flip_noise[0]), NEVER)
    fields = terms.astype(jnp.float32).sum(axis=0)
    own_spins = own_piece(spin_init).astype(jnp.float32)
    own_spins = metropolis(own_spins, fields, limit, first_slot)

    rows = sent_to_all(own_spins.astype(jnp.bfloat16), ("xl", "z"))
    rows = rows.transpose(1, 0, 2).reshape(rep_dev, -1)
    partial = jnp.dot(rows, own_block, preferred_element_type=jnp.float32)
    partial = jnp.concatenate(
        [partial, own_spins, jnp.zeros((rep_dev, 128 - piece), jnp.float32)], axis=1
    )
    partial = lax.all_to_all(
        partial.reshape(n_xl * n_y, share, row_width + 128), PLANE, 0, 0, tiled=True
    )
    fields = partial[:, :, :row_width].reshape(n_xl, n_y, share, row_width).sum(axis=1)
    fields = fields.transpose(1, 0, 2).reshape(share, width)
    spins = partial[:, :, row_width : row_width + piece]
    spins = spins.transpose(1, 0, 2).reshape(share, width)

    steps = jnp.arange(1, SWEEPS, dtype=jnp.int32)[:, None, None]

    def limits_of(xl):
        first = (xl * n_y + y_index) * share
        noise = lax.dynamic_slice_in_dim(flip_noise, first, share, 1)[1:]
        return jnp.where(colors[None, None, :] == steps % 2, noise, NEVER)

    kept = limits_of(xl_index)
    other = lax.ppermute(limits_of(1 - xl_index), "xl", [(0, 1), (1, 0)])
    is_left = xl_index == 0
    limits = jnp.concatenate(
        [jnp.where(is_left, kept, other), jnp.where(is_left, other, kept)], axis=2
    )
    own_slot = first_slot + lax.axis_index(PLANE) * share

    def layer_rows(spins):
        return sent_to_all(spins.astype(jnp.bfloat16), "z")

    def layer_fields(rows, layer_block):
        rows = rows.transpose(1, 0, 2).reshape(share, N)
        halves = [jnp.dot(rows, half, preferred_element_type=jnp.float32) for half in layer_block]
        return jnp.concatenate(halves, axis=1)

    spins = metropolis(spins, fields, limits[0], own_slot)
    rows, gathered = lax.optimization_barrier((layer_rows(spins), gathered))
    layer_block = in_spin_order(
        gathered.reshape(n_core, n_xl, n_y, n_z, piece, row_width)
    )
    for limit in limits[1:]:
        spins = metropolis(spins, layer_fields(rows, layer_block), limit, own_slot)
        spins = lax.optimization_barrier(spins)
        rows = layer_rows(spins)

    layer_sum = jnp.sum(spins * layer_fields(rows, layer_block), axis=1, keepdims=True)
    layer_sum = jnp.broadcast_to(layer_sum, (share, 128))
    energy = -0.5 * sent_to_all(layer_sum, "z").sum(axis=0)

    high = lax.reduce_precision(energy, 8, 7)
    middle = lax.reduce_precision(energy - high, 8, 7)
    low = (energy - high) - middle
    terms = jnp.concatenate(
        [high[:, :1], middle[:, :1], low[:, :1], jnp.zeros((share, 125), jnp.float32)], axis=1
    )
    blocks = spins.astype(jnp.bfloat16).reshape(share, n_xl, row_width).transpose(1, 0, 2)
    terms = jnp.broadcast_to(terms.astype(jnp.bfloat16)[None], (n_xl, share, 128))
    blocks = jnp.concatenate([blocks, terms], axis=2)
    blocks = jnp.broadcast_to(
        blocks[None, :, None], (lax.axis_size(GROUP), n_xl, n_y, *blocks.shape[1:])
    ).reshape(-1, *blocks.shape[1:])
    table = lax.all_to_all(blocks, LAYER, 0, 0, tiled=True).reshape(-1, row_width + 128)

    own_rows = lax.dynamic_slice_in_dim(table, first_slot, rep_dev, 0)
    own_rows = own_rows.astype(jnp.float32)
    mate_rows = jnp.dot(mate_rows_of, table, preferred_element_type=jnp.float32)

    def energy_of(rows):
        return rows[:, row_width] + (rows[:, row_width + 1] + rows[:, row_width + 2])

    own_energy = energy_of(own_rows)
    mate_energy = energy_of(mate_rows)
    swap_gain = beta_gap * (own_energy - mate_energy) * (1.0 / (64.0 * N * math.sqrt(N)))
    accept = swap_gain + noise > 0.0
    spins_out = jnp.where(
        accept[:, None], mate_rows[:, :row_width], own_rows[:, :row_width]
    )
    energies = jnp.where(accept, mate_energy, own_energy) * (1.0 / (N * math.sqrt(N)))
    return (spins_out.astype(jnp.bfloat16), energies)


def solution(mesh):
    fine = Mesh(mesh.devices.reshape(2, 2, 2, 16, 4), ("xh", "core", "xl", "z", "y"))
    rep, row, col = ("xh", "core"), ("xl", "z"), "y"
    in_specs = (
        P(rep, row),
        P(None, col, None, row),
        P(None, rep, row),
        P(row),
        P(),
        P(),
        P(),
    )
    out_specs = (P(rep, row), P(rep))
    return jax.shard_map(
        per_device, mesh=fine, in_specs=in_specs, out_specs=out_specs, check_vma=False
    )
```

```python
import math

import jax
import jax.numpy as jnp
from jax import lax
from jax.experimental import pallas as pl
from jax.experimental.pallas import tpu as pltpu
from jax.sharding import Mesh, PartitionSpec as P

N = 8192
SWEEPS = 10
NEVER = -3.0e38

GROUP = ("xh", "core")
PLANE = ("xl", "y")
LAYER = ("xh", "core", "xl", "y")


def sent_to_all(value, axes):
    length = lax.axis_size(axes)
    return lax.all_to_all(
        jnp.broadcast_to(value[None], (length, *value.shape)), axes, 0, 0, tiled=True
    )


def placed(name, places, pieces, outs):
    def body(scalars, *refs):
        sources, targets, sems = refs[: len(pieces)], refs[len(pieces) : -1], refs[-1]
        copies = [
            pltpu.make_async_copy(sources[i].at[src], targets[o].at[index], sems.at[n])
            for n, (i, src, o, index) in enumerate(places["of"](scalars))
        ]
        for copy in copies:
            copy.start()
        for copy in copies:
            copy.wait()

    return pl.pallas_call(
        body,
        in_specs=[pl.BlockSpec(memory_space=pltpu.SMEM)]
        + [pl.BlockSpec(memory_space=pl.ANY)] * len(pieces),
        out_specs=[pl.BlockSpec(memory_space=pl.ANY)] * len(outs),
        out_shape=[jax.ShapeDtypeStruct(shape, jnp.bfloat16) for shape in outs],
        scratch_shapes=[pltpu.SemaphoreType.DMA((places["count"],))],
        compiler_params=pltpu.CompilerParams(vmem_limit_bytes=2 * 1024 * 1024),
        name=name,
    )(places["scalars"], *pieces)


def per_device(spin_init, couplings, flip_noise, colors, beta_steps, partners, swap_noise):
    rep_dev, row_width = spin_init.shape
    n_xl = lax.axis_size("xl")
    n_y = lax.axis_size("y")
    n_z = lax.axis_size("z")
    n_core = lax.axis_size("core")
    y_index = lax.axis_index("y")
    xl_index = lax.axis_index("xl")
    core_index = lax.axis_index("core")
    rep_index = lax.axis_index(GROUP)
    share = rep_dev // (n_xl * n_y)
    piece = row_width // n_y
    width = n_xl * row_width
    own_block = couplings.reshape(-1, row_width)

    first_slot = rep_index * rep_dev
    all_betas = beta_steps.astype(jnp.float32)
    all_scales = all_betas * (1.0 / 16384.0)

    def metropolis(spins, fields, limit, first):
        scale = lax.dynamic_slice_in_dim(all_scales, first, spins.shape[0])[:, None]
        energy_cost = scale * (spins * fields)
        return jnp.where(energy_cost < limit, -spins, spins)

    terms = lax.dot_general(
        spin_init, own_block, (((1,), (1,)), ((), ())), preferred_element_type=jnp.float32
    )
    terms = terms.astype(jnp.bfloat16).reshape(rep_dev, -1, piece).transpose(1, 0, 2)
    terms = lax.all_to_all(terms, ("xl", "z"), 0, 0, tiled=True)

    def ring(value, shift):
        return lax.ppermute(value, "y", [(i, (i + shift) % n_y) for i in range(n_y)])

    def swapped(value, axis):
        return lax.ppermute(value, axis, [(0, 1), (1, 0)])

    near = lax.dynamic_slice_in_dim(
        couplings.reshape(n_core, n_z, piece, row_width), core_index, 1, 0
    )[0]
    near_below = ring(near, 1)
    near_above = ring(near, -1)
    far = swapped(near, "xl")
    far_below = ring(far, 1)
    far_above = ring(far, -1)

    slot_ids = first_slot + jnp.arange(rep_dev, dtype=jnp.int32)
    mate_ids = lax.dynamic_slice_in_dim(partners, first_slot, rep_dev)
    all_ids = jnp.arange(partners.shape[0], dtype=jnp.int32)[None, :]

    def picked(values, ids):
        return jnp.sum(jnp.where(ids[:, None] == all_ids, values[None, :], 0.0), axis=1)

    beta_gap = picked(all_betas, slot_ids) - picked(all_betas, mate_ids)
    noise = picked(swap_noise, jnp.minimum(slot_ids, mate_ids))
    mate_rows_of = (mate_ids[:, None] == all_ids).astype(jnp.bfloat16)
    terms, beta_gap, noise, mate_rows_of, near_below, near_above, far = (
        lax.optimization_barrier(
            (terms, beta_gap, noise, mate_rows_of, near_below, near_above, far)
        )
    )

    def own_piece(value):
        return lax.dynamic_slice_in_dim(value, y_index * piece, piece, value.ndim - 1)

    limit = jnp.where(own_piece(colors)[None, :] == 0, own_piece(flip_noise[0]), NEVER)
    fields = terms.astype(jnp.float32).sum(axis=0)
    own_spins = own_piece(spin_init).astype(jnp.float32)
    own_spins = metropolis(own_spins, fields, limit, first_slot)

    rows = sent_to_all(own_spins.astype(jnp.bfloat16), ("xl", "z"))
    near_across = ring(near_below, 1)
    far_across = ring(far_above, -1)
    rows, near_across, far_across = lax.optimization_barrier((rows, near_across, far_across))
    rows = rows.transpose(1, 0, 2).reshape(rep_dev, -1)
    partial = jnp.dot(rows, own_block, preferred_element_type=jnp.float32)
    partial = jnp.concatenate(
        [partial, own_spins, jnp.zeros((rep_dev, 128 - piece), jnp.float32)], axis=1
    )
    partial = lax.all_to_all(
        partial.reshape(n_xl * n_y, share, row_width + 128), PLANE, 0, 0, tiled=True
    )
    core_block = (n_z, n_y, piece, row_width)

    def by_y(scalars):
        here = scalars[0]
        shifts = (0, n_y - 1, 1, 2)
        return [
            (side * n_y + n, pl.ds(0, n_z), 0, (side, pl.ds(0, n_z), (here + shift) % n_y))
            for side in range(n_xl)
            for n, shift in enumerate(shifts)
        ]

    (core_half,) = placed(
        "by_y",
        {"of": by_y, "count": n_xl * n_y, "scalars": y_index[None]},
        [near, near_below, near_above, near_across, far, far_below, far_above, far_across],
        [(n_xl, *core_block)],
    )
    other_half = swapped(core_half, "core")

    is_left = xl_index == 0

    def own_first(left, right):
        return jnp.concatenate(
            [jnp.where(is_left, left, right), jnp.where(is_left, right, left)], axis=-1
        )

    fields = partial[:, :, :row_width].reshape(n_xl, n_y, share, row_width).sum(axis=1)
    fields = own_first(fields[0], fields[1])
    spins = partial[:, :, row_width : row_width + piece]
    spins = spins.transpose(1, 0, 2).reshape(share, width)
    spins = own_first(spins[:, :row_width], spins[:, row_width:])

    steps = jnp.arange(1, SWEEPS, dtype=jnp.int32)[:, None, None]

    def limits_of(xl):
        first = (xl * n_y + y_index) * share
        noise = lax.dynamic_slice_in_dim(flip_noise, first, share, 1)[1:]
        return jnp.where(colors[None, None, :] == steps % 2, noise, NEVER)

    kept = limits_of(xl_index)
    limits = jnp.concatenate([kept, swapped(limits_of(1 - xl_index), "xl")], axis=2)
    own_slot = first_slot + lax.axis_index(PLANE) * share

    def layer_rows(spins):
        return sent_to_all(spins.astype(jnp.bfloat16), "z")

    def layer_fields(rows, layer_block):
        rows = rows.transpose(1, 0, 2).reshape(share, N)
        halves = [jnp.dot(rows, half, preferred_element_type=jnp.float32) for half in layer_block]
        return jnp.concatenate(halves, axis=1)

    spins = metropolis(spins, fields, limits[0], own_slot)
    rows, core_half, other_half = lax.optimization_barrier(
        (layer_rows(spins), core_half, other_half)
    )

    def by_core(scalars):
        mine = scalars[0]
        return [
            (source, side, side, (pl.ds(0, n_z), (mine + source) % n_core))
            for source in range(n_core)
            for side in range(n_xl)
        ]

    layer_block = placed(
        "by_core",
        {"of": by_core, "count": n_core * n_xl, "scalars": (core_index ^ xl_index)[None]},
        [core_half, other_half],
        [(n_z, n_core, *core_block[1:])] * n_xl,
    )
    layer_block = [half.reshape(N, row_width) for half in layer_block]

    def final_blocks(spins):
        left_right = own_first(spins[:, :row_width], spins[:, row_width:])
        left_right = left_right.astype(jnp.bfloat16).reshape(share, n_xl, row_width)
        return left_right.transpose(1, 0, 2)

    for limit in limits[1:]:
        spins = metropolis(spins, layer_fields(rows, layer_block), limit, own_slot)
        final_spins = final_blocks(spins)
        spins, final_spins = lax.optimization_barrier((spins, final_spins))
        rows = layer_rows(spins)

    layer_sum = jnp.sum(spins * layer_fields(rows, layer_block), axis=1, keepdims=True)
    layer_sum = jnp.broadcast_to(layer_sum, (share, 128))
    energy = -0.5 * sent_to_all(layer_sum, "z").sum(axis=0)

    high = lax.reduce_precision(energy, 8, 7)
    middle = lax.reduce_precision(energy - high, 8, 7)
    low = (energy - high) - middle
    terms = jnp.concatenate(
        [high[:, :1], middle[:, :1], low[:, :1], jnp.zeros((share, 125), jnp.float32)], axis=1
    )
    terms = jnp.broadcast_to(terms.astype(jnp.bfloat16)[None], (n_xl, share, 128))
    blocks = jnp.concatenate([final_spins, terms], axis=2)
    blocks = jnp.broadcast_to(
        blocks[None, :, None], (lax.axis_size(GROUP), n_xl, n_y, *blocks.shape[1:])
    ).reshape(-1, *blocks.shape[1:])
    table = lax.all_to_all(blocks, LAYER, 0, 0, tiled=True).reshape(-1, row_width + 128)

    own_rows = lax.dynamic_slice_in_dim(table, first_slot, rep_dev, 0)
    own_rows = own_rows.astype(jnp.float32)
    mate_rows = jnp.dot(mate_rows_of, table, preferred_element_type=jnp.float32)

    def energy_of(rows):
        return rows[:, row_width] + (rows[:, row_width + 1] + rows[:, row_width + 2])

    own_energy = energy_of(own_rows)
    mate_energy = energy_of(mate_rows)
    swap_gain = beta_gap * (own_energy - mate_energy) * (1.0 / (64.0 * N * math.sqrt(N)))
    accept = swap_gain + noise > 0.0
    spins_out = jnp.where(
        accept[:, None], mate_rows[:, :row_width], own_rows[:, :row_width]
    )
    energies = jnp.where(accept, mate_energy, own_energy) * (1.0 / (N * math.sqrt(N)))
    return (spins_out.astype(jnp.bfloat16), energies)


def solution(mesh):
    fine = Mesh(mesh.devices.reshape(2, 2, 2, 16, 4), ("xh", "core", "xl", "z", "y"))
    rep, row, col = ("xh", "core"), ("xl", "z"), "y"
    in_specs = (
        P(rep, row),
        P(None, col, None, row),
        P(None, rep, row),
        P(row),
        P(),
        P(),
        P(),
    )
    out_specs = (P(rep, row), P(rep))
    return jax.shard_map(
        per_device, mesh=fine, in_specs=in_specs, out_specs=out_specs, check_vma=False
    )
```

```python
import math

import jax
import jax.numpy as jnp
from jax import lax
from jax.experimental import pallas as pl
from jax.experimental.pallas import tpu as pltpu
from jax.sharding import Mesh, PartitionSpec as P

N = 8192
SWEEPS = 10
NEVER = -3.0e38

GROUP = ("xh", "core")
PLANE = ("xl", "y")
LAYER = ("xh", "core", "xl", "y")


def sent_to_all(value, axes):
    length = lax.axis_size(axes)
    return lax.all_to_all(
        jnp.broadcast_to(value[None], (length, *value.shape)), axes, 0, 0, tiled=True
    )


def in_spin_order(gathered):
    n_core, n_xl, n_y, n_z, piece, width = gathered.shape
    shape = (n_z, n_core * n_y, piece, n_xl * width)

    def body(source, target, sems):
        copies = [
            pltpu.make_async_copy(
                source.at[core, xl, y],
                target.at[:, core * n_y + y, :, pl.ds(xl * width, width)],
                sems.at[core, xl, y],
            )
            for xl in range(n_xl)
            for core in range(n_core)
            for y in range(n_y)
        ]
        for copy in copies:
            copy.start()
        for copy in copies:
            copy.wait()

    ordered = pl.pallas_call(
        body,
        in_specs=[pl.BlockSpec(memory_space=pltpu.HBM)],
        out_specs=pl.BlockSpec(memory_space=pl.ANY),
        out_shape=jax.ShapeDtypeStruct(shape, gathered.dtype),
        scratch_shapes=[pltpu.SemaphoreType.DMA((n_core, n_xl, n_y))],
        compiler_params=pltpu.CompilerParams(vmem_limit_bytes=2 * 1024 * 1024),
        name="in_spin_order",
    )(pltpu.with_memory_space_constraint(gathered, pltpu.HBM))
    return ordered.reshape(-1, n_xl * width)


def left_lanes(shape):
    return lax.broadcasted_iota(jnp.int32, shape, len(shape) - 1) < shape[-1] // 2


def packed(value):
    half = value.shape[0] // 2
    return jnp.concatenate([value[:half], value[half:]], axis=1)


def first_terms(spins, blocks, core, count):
    n_core, rows, width = blocks.shape
    half = spins.shape[0] // 2
    lanes = 2 * (n_core * rows // count)
    pairs = count // 2 // n_core

    def body(core_ref, spins_ref, blocks_ref, out_ref, half_ref, held_ref, sems):
        arrive = [
            pltpu.make_async_copy(blocks_ref.at[n], held_ref.at[n], sems.at[n])
            for n in range(n_core)
        ]
        for copy in arrive:
            copy.start()
        for copy in arrive:
            copy.wait()
        leave = pltpu.make_async_copy(held_ref.at[core_ref[0]], half_ref, sems.at[n_core])
        leave.start()
        is_left = left_lanes((half, lanes))
        for n in range(n_core):
            terms = lax.dot_general(
                spins_ref[...],
                held_ref[n],
                (((1,), (1,)), ((), ())),
                preferred_element_type=jnp.float32,
            )
            for pair in range(pairs):
                both = terms[:, pair * lanes : (pair + 1) * lanes]
                top, bottom = both[:half], both[half:]
                even = jnp.where(is_left, top, pltpu.roll(bottom, lanes // 2, 1))
                odd = jnp.where(is_left, pltpu.roll(top, lanes // 2, 1), bottom)
                at = 2 * (n * pairs + pair)
                out_ref[at] = even.astype(jnp.bfloat16)
                out_ref[at + 1] = odd.astype(jnp.bfloat16)
        leave.wait()

    return pl.pallas_call(
        body,
        in_specs=[
            pl.BlockSpec(memory_space=pltpu.SMEM),
            pl.BlockSpec(memory_space=pltpu.VMEM),
            pl.BlockSpec(memory_space=pl.ANY),
        ],
        out_specs=[pl.BlockSpec(memory_space=pltpu.VMEM), pl.BlockSpec(memory_space=pl.ANY)],
        out_shape=[
            jax.ShapeDtypeStruct((count, half, lanes), jnp.bfloat16),
            jax.ShapeDtypeStruct((rows, width), jnp.bfloat16),
        ],
        scratch_shapes=[
            pltpu.VMEM((n_core, rows, width), jnp.bfloat16),
            pltpu.SemaphoreType.DMA((n_core + 1,)),
        ],
        compiler_params=pltpu.CompilerParams(vmem_limit_bytes=16 * 1024 * 1024),
        name="first_terms",
    )(core[None], spins, pltpu.with_memory_space_constraint(blocks, pltpu.HBM))


def second_terms(rows, own_spins, block, parts):
    count, half, lanes = rows.shape
    width = block.shape[1]
    share = 2 * half // parts

    def body(rows_ref, own_ref, block_ref, out_ref, all_ref, held_ref, sem):
        arrive = pltpu.make_async_copy(block_ref, held_ref, sem)
        arrive.start()
        is_left = left_lanes((half, lanes))
        for pair in range(count // 2):
            even = rows_ref[2 * pair].astype(jnp.float32)
            odd = rows_ref[2 * pair + 1].astype(jnp.float32)
            top = jnp.where(is_left, even, pltpu.roll(odd, lanes // 2, 1))
            bottom = jnp.where(is_left, pltpu.roll(even, lanes // 2, 1), odd)
            at = pl.ds(pair * lanes, lanes)
            all_ref[0:half, at] = top.astype(jnp.bfloat16)
            all_ref[half : 2 * half, at] = bottom.astype(jnp.bfloat16)
        arrive.wait()
        terms = jnp.dot(all_ref[...], held_ref[...], preferred_element_type=jnp.float32)
        out_ref[:, :, 0:width] = terms.reshape(parts, share, width)
        own = own_ref[...]
        beside = pl.ds(width, lanes)
        out_ref[0 : parts // 2, :, beside] = own.reshape(parts // 2, share, lanes)
        own = pltpu.roll(own, lanes // 2, 1)
        out_ref[parts // 2 : parts, :, beside] = own.reshape(parts // 2, share, lanes)

    return pl.pallas_call(
        body,
        out_shape=jax.ShapeDtypeStruct((parts, share, width + lanes), jnp.float32),
        in_specs=[
            pl.BlockSpec(memory_space=pltpu.VMEM),
            pl.BlockSpec(memory_space=pltpu.VMEM),
            pl.BlockSpec(memory_space=pl.ANY),
        ],
        scratch_shapes=[
            pltpu.VMEM((2 * half, block.shape[0]), jnp.bfloat16),
            pltpu.VMEM(block.shape, jnp.bfloat16),
            pltpu.SemaphoreType.DMA,
        ],
        compiler_params=pltpu.CompilerParams(vmem_limit_bytes=16 * 1024 * 1024),
        name="second_terms",
    )(rows, own_spins, pltpu.with_memory_space_constraint(block, pltpu.HBM))


def per_device(spin_init, couplings, flip_noise, colors, beta_steps, partners, swap_noise):
    rep_dev, row_width = spin_init.shape
    n_xl = lax.axis_size("xl")
    n_y = lax.axis_size("y")
    n_z = lax.axis_size("z")
    n_core = lax.axis_size("core")
    y_index = lax.axis_index("y")
    xl_index = lax.axis_index("xl")
    core_index = lax.axis_index("core")
    rep_index = lax.axis_index(GROUP)
    share = rep_dev // (n_xl * n_y)
    piece = row_width // n_y
    width = n_xl * row_width
    own_block = couplings.reshape(-1, row_width)

    first_slot = rep_index * rep_dev

    def metropolis(spins, fields, limit, scale):
        energy_cost = scale * (spins * fields)
        return jnp.where(energy_cost < limit, -spins, spins)

    terms, core_half = first_terms(
        spin_init, own_block.reshape(n_core, -1, row_width), core_index, n_xl * n_z
    )
    gathered = lax.all_gather(core_half, ("core", *PLANE))
    terms = lax.all_to_all(terms, ("xl", "z"), 0, 0, tiled=True)
    all_betas = beta_steps.astype(jnp.float32)
    all_scales = all_betas * (1.0 / 16384.0)

    def scales(first, length):
        return lax.dynamic_slice_in_dim(all_scales, first, length)[:, None]

    slot_ids = first_slot + jnp.arange(rep_dev, dtype=jnp.int32)
    mate_ids = lax.dynamic_slice_in_dim(partners, first_slot, rep_dev)
    all_ids = jnp.arange(partners.shape[0], dtype=jnp.int32)[None, :]

    def picked(values, ids):
        return jnp.sum(jnp.where(ids[:, None] == all_ids, values[None, :], 0.0), axis=1)

    beta_gap = picked(all_betas, slot_ids) - picked(all_betas, mate_ids)
    noise = picked(swap_noise, jnp.minimum(slot_ids, mate_ids))
    mate_rows_of = (mate_ids[:, None] == all_ids).astype(jnp.bfloat16)

    def own_piece(value):
        return lax.dynamic_slice_in_dim(value, y_index * piece, piece, value.ndim - 1)

    limit = jnp.where(own_piece(colors)[None, :] == 0, own_piece(flip_noise[0]), NEVER)
    fields = terms.astype(jnp.float32).sum(axis=0)
    own_spins = packed(own_piece(spin_init)).astype(jnp.float32)
    own_scales = packed(jnp.broadcast_to(scales(first_slot, rep_dev), (rep_dev, piece)))
    own_spins = metropolis(own_spins, fields, packed(limit), own_scales)
    own_spins, late_noise, late_colors = lax.optimization_barrier(
        (own_spins, flip_noise, colors)
    )

    rows = sent_to_all(own_spins.astype(jnp.bfloat16), ("xl", "z"))

    def limits_of(xl):
        first = (xl * n_y + y_index) * share
        noise = lax.dynamic_slice_in_dim(late_noise, first, share, 1)
        return [
            jnp.where(late_colors[None, :] == step % 2, noise[step], NEVER)
            for step in range(1, SWEEPS)
        ]

    is_left = xl_index == 0
    kept = limits_of(xl_index)
    other = lax.ppermute(jnp.stack(limits_of(1 - xl_index)), "xl", [(0, 1), (1, 0)])
    limits = [
        jnp.concatenate(
            [jnp.where(is_left, here, there), jnp.where(is_left, there, here)], axis=1
        )
        for here, there in zip(kept, other)
    ]
    scale = scales(first_slot + lax.axis_index(PLANE) * share, share)

    partial = second_terms(rows, own_spins, own_block, n_xl * n_y)
    partial, limits, scale, beta_gap, noise, mate_rows_of = lax.optimization_barrier(
        (partial, limits, scale, beta_gap, noise, mate_rows_of)
    )
    partial = lax.all_to_all(partial, PLANE, 0, 0, tiled=True)
    fields = partial[:, :, :row_width].reshape(n_xl, n_y, share, row_width).sum(axis=1)
    fields = fields.transpose(1, 0, 2).reshape(share, width)
    spins = partial[:, :, row_width : row_width + piece]
    spins = spins.transpose(1, 0, 2).reshape(share, width)

    def layer_rows(spins):
        return sent_to_all(spins.astype(jnp.bfloat16), "z")

    def layer_fields(rows, layer_block):
        rows = rows.transpose(1, 0, 2).reshape(share, N)
        return jnp.dot(rows, layer_block, preferred_element_type=jnp.float32)

    spins = metropolis(spins, fields, limits[0], scale)
    spins = lax.optimization_barrier(spins)
    rows, gathered = lax.optimization_barrier((layer_rows(spins), gathered))
    layer_block = in_spin_order(
        gathered.reshape(n_core, n_xl, n_y, n_z, piece, row_width)
    )
    for limit in limits[1:]:
        spins = metropolis(spins, layer_fields(rows, layer_block), limit, scale)
        spins = lax.optimization_barrier(spins)
        rows = layer_rows(spins)

    layer_sum = jnp.sum(spins * layer_fields(rows, layer_block), axis=1, keepdims=True)
    layer_sum = jnp.broadcast_to(layer_sum, (share, 128))
    energy = -0.5 * sent_to_all(layer_sum, "z").sum(axis=0)

    high = lax.reduce_precision(energy, 8, 7)
    middle = lax.reduce_precision(energy - high, 8, 7)
    low = (energy - high) - middle
    terms = jnp.concatenate([high[:, :1], middle[:, :1], low[:, :126]], axis=1)
    blocks = spins.astype(jnp.bfloat16).reshape(share, n_xl, row_width).transpose(1, 0, 2)
    terms = jnp.broadcast_to(terms.astype(jnp.bfloat16)[None], (n_xl, share, 128))
    blocks = jnp.concatenate([blocks, terms], axis=2)
    blocks = jnp.broadcast_to(
        blocks[None, :, None], (lax.axis_size(GROUP), n_xl, n_y, *blocks.shape[1:])
    ).reshape(-1, *blocks.shape[1:])
    table = lax.all_to_all(blocks, LAYER, 0, 0, tiled=True).reshape(-1, row_width + 128)

    own_rows = lax.dynamic_slice_in_dim(table, first_slot, rep_dev, 0)
    own_rows = own_rows.astype(jnp.float32)
    mate_rows = jnp.dot(mate_rows_of, table, preferred_element_type=jnp.float32)

    def energy_of(rows):
        return rows[:, row_width] + (rows[:, row_width + 1] + rows[:, row_width + 2])

    own_energy = energy_of(own_rows)
    mate_energy = energy_of(mate_rows)
    swap_gain = beta_gap * (own_energy - mate_energy) * (1.0 / (64.0 * N * math.sqrt(N)))
    accept = swap_gain + noise > 0.0
    spins_out = jnp.where(
        accept[:, None], mate_rows[:, :row_width], own_rows[:, :row_width]
    )
    energies = jnp.where(accept, mate_energy, own_energy) * (1.0 / (N * math.sqrt(N)))
    return (spins_out.astype(jnp.bfloat16), energies)


def solution(mesh):
    fine = Mesh(mesh.devices.reshape(2, 2, 2, 16, 4), ("xh", "core", "xl", "z", "y"))
    rep, row, col = ("xh", "core"), ("xl", "z"), "y"
    in_specs = (
        P(rep, row),
        P(None, col, None, row),
        P(None, rep, row),
        P(row),
        P(),
        P(),
        P(),
    )
    out_specs = (P(rep, row), P(rep))
    return jax.shard_map(
        per_device, mesh=fine, in_specs=in_specs, out_specs=out_specs, check_vma=False
    )
```

```python
import math

import jax
import jax.numpy as jnp
from jax import lax
from jax.experimental import pallas as pl
from jax.experimental.pallas import tpu as pltpu
from jax.sharding import Mesh, PartitionSpec as P

N = 8192
SWEEPS = 10
NEVER = -3.0e38

GROUP = ("xh", "core")
PLANE = ("xl", "y")
LAYER = ("xh", "core", "xl", "y")


def sent_to_all(value, axes):
    length = lax.axis_size(axes)
    return lax.all_to_all(
        jnp.broadcast_to(value[None], (length, *value.shape)), axes, 0, 0, tiled=True
    )


def in_spin_order(gathered):
    n_core, n_xl, n_y, n_z, piece, width = gathered.shape
    shape = (n_z, n_core * n_y, piece, n_xl * width)

    def body(source, target, sems):
        copies = [
            pltpu.make_async_copy(
                source.at[core, xl, y],
                target.at[:, core * n_y + y, :, pl.ds(xl * width, width)],
                sems.at[core, xl, y],
            )
            for xl in range(n_xl)
            for core in range(n_core)
            for y in range(n_y)
        ]
        for copy in copies:
            copy.start()
        for copy in copies:
            copy.wait()

    ordered = pl.pallas_call(
        body,
        in_specs=[pl.BlockSpec(memory_space=pltpu.HBM)],
        out_specs=pl.BlockSpec(memory_space=pl.ANY),
        out_shape=jax.ShapeDtypeStruct(shape, gathered.dtype),
        scratch_shapes=[pltpu.SemaphoreType.DMA((n_core, n_xl, n_y))],
        compiler_params=pltpu.CompilerParams(vmem_limit_bytes=2 * 1024 * 1024),
        name="in_spin_order",
    )(pltpu.with_memory_space_constraint(gathered, pltpu.HBM))
    return ordered.reshape(-1, n_xl * width)


def left_lanes(shape):
    return lax.broadcasted_iota(jnp.int32, shape, len(shape) - 1) < shape[-1] // 2


def packed(value):
    half = value.shape[0] // 2
    return jnp.concatenate([value[:half], value[half:]], axis=1)


def first_terms(spins, blocks, core, count):
    n_core, rows, width = blocks.shape
    half = spins.shape[0] // 2
    lanes = 2 * (n_core * rows // count)
    pairs = count // 2 // n_core

    def body(core_ref, spins_ref, blocks_ref, out_ref, half_ref, held_ref, sems):
        arrive = [
            pltpu.make_async_copy(blocks_ref.at[n], held_ref.at[n], sems.at[n])
            for n in range(n_core)
        ]
        for copy in arrive:
            copy.start()
        for copy in arrive:
            copy.wait()
        leave = pltpu.make_async_copy(held_ref.at[core_ref[0]], half_ref, sems.at[n_core])
        leave.start()
        is_left = left_lanes((half, lanes))
        for n in range(n_core):
            terms = lax.dot_general(
                spins_ref[...],
                held_ref[n],
                (((1,), (1,)), ((), ())),
                preferred_element_type=jnp.float32,
            )
            for pair in range(pairs):
                both = terms[:, pair * lanes : (pair + 1) * lanes]
                top, bottom = both[:half], both[half:]
                even = jnp.where(is_left, top, pltpu.roll(bottom, lanes // 2, 1))
                odd = jnp.where(is_left, pltpu.roll(top, lanes // 2, 1), bottom)
                at = 2 * (n * pairs + pair)
                out_ref[at] = even.astype(jnp.bfloat16)
                out_ref[at + 1] = odd.astype(jnp.bfloat16)
        leave.wait()

    return pl.pallas_call(
        body,
        in_specs=[
            pl.BlockSpec(memory_space=pltpu.SMEM),
            pl.BlockSpec(memory_space=pltpu.VMEM),
            pl.BlockSpec(memory_space=pl.ANY),
        ],
        out_specs=[pl.BlockSpec(memory_space=pltpu.VMEM), pl.BlockSpec(memory_space=pl.ANY)],
        out_shape=[
            jax.ShapeDtypeStruct((count, half, lanes), jnp.bfloat16),
            jax.ShapeDtypeStruct((rows, width), jnp.bfloat16),
        ],
        scratch_shapes=[
            pltpu.VMEM((n_core, rows, width), jnp.bfloat16),
            pltpu.SemaphoreType.DMA((n_core + 1,)),
        ],
        compiler_params=pltpu.CompilerParams(vmem_limit_bytes=16 * 1024 * 1024),
        name="first_terms",
    )(core[None], spins, pltpu.with_memory_space_constraint(blocks, pltpu.HBM))


def second_terms(rows, own_spins, block, parts):
    count, half, lanes = rows.shape
    width = block.shape[1]
    share = 2 * half // parts

    def body(rows_ref, own_ref, block_ref, out_ref, all_ref, held_ref, sem):
        arrive = pltpu.make_async_copy(block_ref, held_ref, sem)
        arrive.start()
        is_left = left_lanes((half, lanes))
        for pair in range(count // 2):
            even = rows_ref[2 * pair].astype(jnp.float32)
            odd = rows_ref[2 * pair + 1].astype(jnp.float32)
            top = jnp.where(is_left, even, pltpu.roll(odd, lanes // 2, 1))
            bottom = jnp.where(is_left, pltpu.roll(even, lanes // 2, 1), odd)
            at = pl.ds(pair * lanes, lanes)
            all_ref[0:half, at] = top.astype(jnp.bfloat16)
            all_ref[half : 2 * half, at] = bottom.astype(jnp.bfloat16)
        arrive.wait()
        terms = jnp.dot(all_ref[...], held_ref[...], preferred_element_type=jnp.float32)
        out_ref[:, :, 0:width] = terms.reshape(parts, share, width)
        own = own_ref[...]
        beside = pl.ds(width, lanes)
        out_ref[0 : parts // 2, :, beside] = own.reshape(parts // 2, share, lanes)
        own = pltpu.roll(own, lanes // 2, 1)
        out_ref[parts // 2 : parts, :, beside] = own.reshape(parts // 2, share, lanes)

    return pl.pallas_call(
        body,
        out_shape=jax.ShapeDtypeStruct((parts, share, width + lanes), jnp.float32),
        in_specs=[
            pl.BlockSpec(memory_space=pltpu.VMEM),
            pl.BlockSpec(memory_space=pltpu.VMEM),
            pl.BlockSpec(memory_space=pl.ANY),
        ],
        scratch_shapes=[
            pltpu.VMEM((2 * half, block.shape[0]), jnp.bfloat16),
            pltpu.VMEM(block.shape, jnp.bfloat16),
            pltpu.SemaphoreType.DMA,
        ],
        compiler_params=pltpu.CompilerParams(vmem_limit_bytes=16 * 1024 * 1024),
        name="second_terms",
    )(rows, own_spins, pltpu.with_memory_space_constraint(block, pltpu.HBM))


def per_device(spin_init, couplings, flip_noise, colors, beta_steps, partners, swap_noise):
    rep_dev, row_width = spin_init.shape
    n_xl = lax.axis_size("xl")
    n_y = lax.axis_size("y")
    n_z = lax.axis_size("z")
    n_core = lax.axis_size("core")
    y_index = lax.axis_index("y")
    xl_index = lax.axis_index("xl")
    core_index = lax.axis_index("core")
    rep_index = lax.axis_index(GROUP)
    share = rep_dev // (n_xl * n_y)
    piece = row_width // n_y
    width = n_xl * row_width
    own_block = couplings.reshape(-1, row_width)

    first_slot = rep_index * rep_dev

    def metropolis(spins, fields, limit, scale):
        energy_cost = scale * (spins * fields)
        return jnp.where(energy_cost < limit, -spins, spins)

    terms, core_half = first_terms(
        spin_init, own_block.reshape(n_core, -1, row_width), core_index, n_xl * n_z
    )
    gathered = lax.all_gather(core_half, ("core", *PLANE))
    terms = lax.all_to_all(terms, ("xl", "z"), 0, 0, tiled=True)
    all_betas = beta_steps.astype(jnp.float32)
    all_scales = all_betas * (1.0 / 16384.0)

    def scales(first, length):
        return lax.dynamic_slice_in_dim(all_scales, first, length)[:, None]

    slot_ids = first_slot + jnp.arange(rep_dev, dtype=jnp.int32)
    mate_ids = lax.dynamic_slice_in_dim(partners, first_slot, rep_dev)
    all_ids = jnp.arange(partners.shape[0], dtype=jnp.int32)[None, :]

    def picked(values, ids):
        return jnp.sum(jnp.where(ids[:, None] == all_ids, values[None, :], 0.0), axis=1)

    beta_gap = picked(all_betas, slot_ids) - picked(all_betas, mate_ids)
    noise = picked(swap_noise, jnp.minimum(slot_ids, mate_ids))
    mate_rows_of = (mate_ids[:, None] == all_ids).astype(jnp.bfloat16)

    def own_piece(value):
        return lax.dynamic_slice_in_dim(value, y_index * piece, piece, value.ndim - 1)

    limit = jnp.where(own_piece(colors)[None, :] == 0, own_piece(flip_noise[0]), NEVER)
    fields = terms.astype(jnp.float32).sum(axis=0)
    own_spins = packed(own_piece(spin_init)).astype(jnp.float32)
    own_scales = packed(jnp.broadcast_to(scales(first_slot, rep_dev), (rep_dev, piece)))
    own_spins = metropolis(own_spins, fields, packed(limit), own_scales)
    own_spins = lax.optimization_barrier(own_spins)

    rows = sent_to_all(own_spins.astype(jnp.bfloat16), ("xl", "z"))

    steps = jnp.arange(1, SWEEPS, dtype=jnp.int32)[:, None, None]

    def limits_of(xl):
        first = (xl * n_y + y_index) * share
        noise = lax.dynamic_slice_in_dim(flip_noise, first, share, 1)[1:]
        return jnp.where(colors[None, None, :] == steps % 2, noise, NEVER)

    is_left = xl_index == 0
    kept = limits_of(xl_index)
    other = limits_of(1 - xl_index)
    other = lax.ppermute(other, "xl", [(0, 1), (1, 0)])
    limits = jnp.concatenate(
        [jnp.where(is_left, kept, other), jnp.where(is_left, other, kept)], axis=2
    )
    limits = [limits[step] for step in range(SWEEPS - 1)]
    scale = scales(first_slot + lax.axis_index(PLANE) * share, share)

    partial = second_terms(rows, own_spins, own_block, n_xl * n_y)
    partial, limits, scale, beta_gap, noise, mate_rows_of = lax.optimization_barrier(
        (partial, limits, scale, beta_gap, noise, mate_rows_of)
    )
    partial = lax.all_to_all(partial, PLANE, 0, 0, tiled=True)
    fields = partial[:, :, :row_width].reshape(n_xl, n_y, share, row_width).sum(axis=1)
    fields = fields.transpose(1, 0, 2).reshape(share, width)
    spins = partial[:, :, row_width : row_width + piece]
    spins = spins.transpose(1, 0, 2).reshape(share, width)

    def layer_rows(spins):
        return sent_to_all(spins.astype(jnp.bfloat16), "z")

    def layer_fields(rows, layer_block):
        rows = rows.transpose(1, 0, 2).reshape(share, N)
        return jnp.dot(rows, layer_block, preferred_element_type=jnp.float32)

    spins = metropolis(spins, fields, limits[0], scale)
    spins = lax.optimization_barrier(spins)
    rows, gathered = lax.optimization_barrier((layer_rows(spins), gathered))
    layer_block = in_spin_order(
        gathered.reshape(n_core, n_xl, n_y, n_z, piece, row_width)
    )
    for limit in limits[1:]:
        spins = metropolis(spins, layer_fields(rows, layer_block), limit, scale)
        spins = lax.optimization_barrier(spins)
        rows = layer_rows(spins)

    layer_sum = jnp.sum(spins * layer_fields(rows, layer_block), axis=1, keepdims=True)
    layer_sum = jnp.broadcast_to(layer_sum, (share, 128))
    energy = -0.5 * sent_to_all(layer_sum, "z").sum(axis=0)

    high = lax.reduce_precision(energy, 8, 7)
    middle = lax.reduce_precision(energy - high, 8, 7)
    low = (energy - high) - middle
    terms = jnp.concatenate([high[:, :1], middle[:, :1], low[:, :126]], axis=1)
    blocks = spins.astype(jnp.bfloat16).reshape(share, n_xl, row_width).transpose(1, 0, 2)
    terms = jnp.broadcast_to(terms.astype(jnp.bfloat16)[None], (n_xl, share, 128))
    blocks = jnp.concatenate([blocks, terms], axis=2)
    blocks = jnp.broadcast_to(
        blocks[None, :, None], (lax.axis_size(GROUP), n_xl, n_y, *blocks.shape[1:])
    ).reshape(-1, *blocks.shape[1:])
    table = lax.all_to_all(blocks, LAYER, 0, 0, tiled=True).reshape(-1, row_width + 128)

    own_rows = lax.dynamic_slice_in_dim(table, first_slot, rep_dev, 0)
    own_rows = own_rows.astype(jnp.float32)
    mate_rows = jnp.dot(mate_rows_of, table, preferred_element_type=jnp.float32)

    def energy_of(rows):
        return rows[:, row_width] + (rows[:, row_width + 1] + rows[:, row_width + 2])

    own_energy = energy_of(own_rows)
    mate_energy = energy_of(mate_rows)
    swap_gain = beta_gap * (own_energy - mate_energy) * (1.0 / (64.0 * N * math.sqrt(N)))
    accept = swap_gain + noise > 0.0
    spins_out = jnp.where(
        accept[:, None], mate_rows[:, :row_width], own_rows[:, :row_width]
    )
    energies = jnp.where(accept, mate_energy, own_energy) * (1.0 / (N * math.sqrt(N)))
    return (spins_out.astype(jnp.bfloat16), energies)


def solution(mesh):
    fine = Mesh(mesh.devices.reshape(2, 2, 2, 16, 4), ("xh", "core", "xl", "z", "y"))
    rep, row, col = ("xh", "core"), ("xl", "z"), "y"
    in_specs = (
        P(rep, row),
        P(None, col, None, row),
        P(None, rep, row),
        P(row),
        P(),
        P(),
        P(),
    )
    out_specs = (P(rep, row), P(rep))
    return jax.shard_map(
        per_device, mesh=fine, in_specs=in_specs, out_specs=out_specs, check_vma=False
    )
```

```python
import math

import jax
import jax.numpy as jnp
from jax import lax
from jax.experimental import pallas as pl
from jax.experimental.pallas import tpu as pltpu
from jax.sharding import Mesh, PartitionSpec as P

N = 8192
SWEEPS = 10
NEVER = -3.0e38

GROUP = ("xh", "core")
PLANE = ("xl", "y")
LAYER = ("xh", "core", "xl", "y")


def sent_to_all(value, axes):
    length = lax.axis_size(axes)
    return lax.all_to_all(
        jnp.broadcast_to(value[None], (length, *value.shape)), axes, 0, 0, tiled=True
    )


def in_spin_order(gathered):
    n_core, n_xl, n_y, n_z, piece, width = gathered.shape
    shape = (n_z, n_core * n_y, piece, n_xl * width)

    def body(source, target, sems):
        copies = [
            pltpu.make_async_copy(
                source.at[core, xl, y],
                target.at[:, core * n_y + y, :, pl.ds(xl * width, width)],
                sems.at[core, xl, y],
            )
            for xl in range(n_xl)
            for core in range(n_core)
            for y in range(n_y)
        ]
        for copy in copies:
            copy.start()
        for copy in copies:
            copy.wait()

    ordered = pl.pallas_call(
        body,
        in_specs=[pl.BlockSpec(memory_space=pltpu.HBM)],
        out_specs=pl.BlockSpec(memory_space=pl.ANY),
        out_shape=jax.ShapeDtypeStruct(shape, gathered.dtype),
        scratch_shapes=[pltpu.SemaphoreType.DMA((n_core, n_xl, n_y))],
        compiler_params=pltpu.CompilerParams(vmem_limit_bytes=2 * 1024 * 1024),
        name="in_spin_order",
    )(pltpu.with_memory_space_constraint(gathered, pltpu.HBM))
    return ordered.reshape(-1, n_xl * width)


def left_lanes(shape):
    return lax.broadcasted_iota(jnp.int32, shape, len(shape) - 1) < shape[-1] // 2


def packed(value):
    half = value.shape[0] // 2
    return jnp.concatenate([value[:half], value[half:]], axis=1)


def first_terms(spins, blocks, core, xl, count):
    n_core, rows, width = blocks.shape
    half = spins.shape[0] // 2
    lanes = 2 * (n_core * rows // count)
    pairs = count // 2 // n_core

    def body(core_ref, xl_ref, spins_ref, blocks_ref, out_ref, one_ref, two_ref, held_ref, sems):
        arrive = [
            pltpu.make_async_copy(blocks_ref.at[n], held_ref.at[n], sems.at[n])
            for n in range(n_core)
        ]
        for copy in arrive:
            copy.start()
        for copy in arrive:
            copy.wait()
        leave = [
            pltpu.make_async_copy(held_ref.at[core_ref[0]], one_ref, sems.at[n_core]),
            pltpu.make_async_copy(held_ref.at[1 - xl_ref[0]], two_ref, sems.at[n_core + 1]),
        ]
        for copy in leave:
            copy.start()
        is_left = left_lanes((half, lanes))
        for n in range(n_core):
            terms = lax.dot_general(
                spins_ref[...],
                held_ref[n],
                (((1,), (1,)), ((), ())),
                preferred_element_type=jnp.float32,
            )
            for pair in range(pairs):
                both = terms[:, pair * lanes : (pair + 1) * lanes]
                top, bottom = both[:half], both[half:]
                even = jnp.where(is_left, top, pltpu.roll(bottom, lanes // 2, 1))
                odd = jnp.where(is_left, pltpu.roll(top, lanes // 2, 1), bottom)
                at = 2 * (n * pairs + pair)
                out_ref[at] = even.astype(jnp.bfloat16)
                out_ref[at + 1] = odd.astype(jnp.bfloat16)
        for copy in leave:
            copy.wait()

    return pl.pallas_call(
        body,
        in_specs=[
            pl.BlockSpec(memory_space=pltpu.SMEM),
            pl.BlockSpec(memory_space=pltpu.SMEM),
            pl.BlockSpec(memory_space=pltpu.VMEM),
            pl.BlockSpec(memory_space=pl.ANY),
        ],
        out_specs=[pl.BlockSpec(memory_space=pltpu.VMEM)]
        + [pl.BlockSpec(memory_space=pl.ANY)] * 2,
        out_shape=[jax.ShapeDtypeStruct((count, half, lanes), jnp.bfloat16)]
        + [jax.ShapeDtypeStruct((rows, width), jnp.bfloat16)] * 2,
        scratch_shapes=[
            pltpu.VMEM((n_core, rows, width), jnp.bfloat16),
            pltpu.SemaphoreType.DMA((n_core + 2,)),
        ],
        compiler_params=pltpu.CompilerParams(vmem_limit_bytes=16 * 1024 * 1024),
        name="first_terms",
    )(core[None], xl[None], spins, pltpu.with_memory_space_constraint(blocks, pltpu.HBM))


def second_terms(rows, own_spins, blocks, own, far, parts):
    count, half, lanes = rows.shape
    depth, width = far.shape
    share = 2 * half // parts

    def body(own_ref, rows_ref, piece_ref, blocks_ref, far_ref, out_ref, all_ref, held_ref, sems):
        arrive = [
            pltpu.make_async_copy(blocks_ref.at[own_ref[0]], held_ref.at[0], sems.at[0]),
            pltpu.make_async_copy(far_ref, held_ref.at[1], sems.at[1]),
        ]
        for copy in arrive:
            copy.start()
        is_left = left_lanes((half, lanes))
        for pair in range(count // 2):
            even = rows_ref[2 * pair].astype(jnp.float32)
            odd = rows_ref[2 * pair + 1].astype(jnp.float32)
            top = jnp.where(is_left, even, pltpu.roll(odd, lanes // 2, 1))
            bottom = jnp.where(is_left, pltpu.roll(even, lanes // 2, 1), odd)
            at = pl.ds(pair * lanes, lanes)
            all_ref[0:half, at] = top.astype(jnp.bfloat16)
            all_ref[half : 2 * half, at] = bottom.astype(jnp.bfloat16)
        piece = piece_ref[...]
        beside = pl.ds(2 * width, lanes)
        out_ref[0 : parts // 2, :, beside] = piece.reshape(parts // 2, share, lanes)
        piece = pltpu.roll(piece, lanes // 2, 1)
        out_ref[parts // 2 : parts, :, beside] = piece.reshape(parts // 2, share, lanes)
        for n, copy in enumerate(arrive):
            copy.wait()
            terms = jnp.dot(all_ref[...], held_ref[n], preferred_element_type=jnp.float32)
            out_ref[:, :, n * width : (n + 1) * width] = terms.reshape(parts, share, width)

    return pl.pallas_call(
        body,
        out_shape=jax.ShapeDtypeStruct((parts, share, 2 * width + lanes), jnp.float32),
        in_specs=[
            pl.BlockSpec(memory_space=pltpu.SMEM),
            pl.BlockSpec(memory_space=pltpu.VMEM),
            pl.BlockSpec(memory_space=pltpu.VMEM),
            pl.BlockSpec(memory_space=pl.ANY),
            pl.BlockSpec(memory_space=pl.ANY),
        ],
        scratch_shapes=[
            pltpu.VMEM((2 * half, depth), jnp.bfloat16),
            pltpu.VMEM((2, depth, width), jnp.bfloat16),
            pltpu.SemaphoreType.DMA((2,)),
        ],
        compiler_params=pltpu.CompilerParams(vmem_limit_bytes=16 * 1024 * 1024),
        name="second_terms",
    )(own[None], rows, own_spins, pltpu.with_memory_space_constraint(blocks, pltpu.HBM), far)


def per_device(spin_init, couplings, flip_noise, colors, beta_steps, partners, swap_noise):
    rep_dev, row_width = spin_init.shape
    n_xl = lax.axis_size("xl")
    n_y = lax.axis_size("y")
    n_z = lax.axis_size("z")
    n_core = lax.axis_size("core")
    y_index = lax.axis_index("y")
    xl_index = lax.axis_index("xl")
    core_index = lax.axis_index("core")
    rep_index = lax.axis_index(GROUP)
    share = rep_dev // (n_xl * n_y)
    piece = row_width // n_y
    width = n_xl * row_width
    own_block = couplings.reshape(-1, row_width)

    first_slot = rep_index * rep_dev

    def metropolis(spins, fields, limit, scale):
        energy_cost = scale * (spins * fields)
        return jnp.where(energy_cost < limit, -spins, spins)

    blocks = own_block.reshape(n_core, -1, row_width)
    terms, core_half, cross = first_terms(
        spin_init, blocks, core_index, xl_index, n_xl * n_z
    )
    gathered = lax.all_gather(core_half, ("core", *PLANE))
    terms = lax.all_to_all(terms, ("xl", "z"), 0, 0, tiled=True)
    far = lax.ppermute(cross, ("xh", "xl"), [(0, 3), (3, 0), (1, 2), (2, 1)])
    all_betas = beta_steps.astype(jnp.float32)
    all_scales = all_betas * (1.0 / 16384.0)

    def scales(first, length):
        return lax.dynamic_slice_in_dim(all_scales, first, length)[:, None]

    slot_ids = first_slot + jnp.arange(rep_dev, dtype=jnp.int32)
    mate_ids = lax.dynamic_slice_in_dim(partners, first_slot, rep_dev)
    all_ids = jnp.arange(partners.shape[0], dtype=jnp.int32)[None, :]

    def picked(values, ids):
        return jnp.sum(jnp.where(ids[:, None] == all_ids, values[None, :], 0.0), axis=1)

    beta_gap = picked(all_betas, slot_ids) - picked(all_betas, mate_ids)
    noise = picked(swap_noise, jnp.minimum(slot_ids, mate_ids))
    mate_rows_of = (mate_ids[:, None] == all_ids).astype(jnp.bfloat16)

    def own_piece(value):
        return lax.dynamic_slice_in_dim(value, y_index * piece, piece, value.ndim - 1)

    limit = jnp.where(own_piece(colors)[None, :] == 0, own_piece(flip_noise[0]), NEVER)
    fields = terms.astype(jnp.float32).sum(axis=0)
    own_spins = packed(own_piece(spin_init)).astype(jnp.float32)
    own_scales = packed(jnp.broadcast_to(scales(first_slot, rep_dev), (rep_dev, piece)))
    own_spins = metropolis(own_spins, fields, packed(limit), own_scales)


    steps = jnp.arange(1, SWEEPS, dtype=jnp.int32)[:, None, None]

    def limits_of(xl):
        first = (xl * n_y + y_index) * share
        noise = lax.dynamic_slice_in_dim(flip_noise, first, share, 1)[1:]
        return jnp.where(colors[None, None, :] == steps % 2, noise, NEVER)

    is_left = xl_index == 0
    kept = limits_of(xl_index)
    other = limits_of(1 - xl_index)
    other = lax.ppermute(other, "xl", [(0, 1), (1, 0)])
    limits = jnp.concatenate(
        [jnp.where(is_left, kept, other), jnp.where(is_left, other, kept)], axis=2
    )
    limits = [limits[step] for step in range(SWEEPS - 1)]
    scale = scales(first_slot + lax.axis_index(PLANE) * share, share)

    own_spins, limits, scale, beta_gap, noise, mate_rows_of = lax.optimization_barrier(
        (own_spins, limits, scale, beta_gap, noise, mate_rows_of)
    )
    rows = sent_to_all(own_spins.astype(jnp.bfloat16), "z")
    partial = second_terms(rows, own_spins, blocks, xl_index, far, n_xl * n_y)
    partial = lax.all_to_all(partial, PLANE, 0, 0, tiled=True)
    fields = partial.reshape(n_xl, n_y, share, -1).sum(axis=1)
    fields = jnp.concatenate(
        [
            fields[side, :, :row_width] + fields[1 - side, :, row_width:width]
            for side in range(n_xl)
        ],
        axis=1,
    )
    spins = partial[:, :, width : width + piece]
    spins = spins.transpose(1, 0, 2).reshape(share, width)

    def layer_rows(spins):
        return sent_to_all(spins.astype(jnp.bfloat16), "z")

    def layer_fields(rows, layer_block):
        rows = rows.transpose(1, 0, 2).reshape(share, N)
        return jnp.dot(rows, layer_block, preferred_element_type=jnp.float32)

    spins = metropolis(spins, fields, limits[0], scale)
    spins = lax.optimization_barrier(spins)
    rows, gathered = lax.optimization_barrier((layer_rows(spins), gathered))
    layer_block = in_spin_order(
        gathered.reshape(n_core, n_xl, n_y, n_z, piece, row_width)
    )
    for limit in limits[1:]:
        spins = metropolis(spins, layer_fields(rows, layer_block), limit, scale)
        spins = lax.optimization_barrier(spins)
        rows = layer_rows(spins)

    layer_sum = jnp.sum(spins * layer_fields(rows, layer_block), axis=1, keepdims=True)
    layer_sum = jnp.broadcast_to(layer_sum, (share, 128))
    energy = -0.5 * sent_to_all(layer_sum, "z").sum(axis=0)

    high = lax.reduce_precision(energy, 8, 7)
    middle = lax.reduce_precision(energy - high, 8, 7)
    low = (energy - high) - middle
    terms = jnp.concatenate([high[:, :1], middle[:, :1], low[:, :126]], axis=1)
    blocks = spins.astype(jnp.bfloat16).reshape(share, n_xl, row_width).transpose(1, 0, 2)
    terms = jnp.broadcast_to(terms.astype(jnp.bfloat16)[None], (n_xl, share, 128))
    blocks = jnp.concatenate([blocks, terms], axis=2)
    blocks = jnp.broadcast_to(
        blocks[None, :, None], (lax.axis_size(GROUP), n_xl, n_y, *blocks.shape[1:])
    ).reshape(-1, *blocks.shape[1:])
    table = lax.all_to_all(blocks, LAYER, 0, 0, tiled=True).reshape(-1, row_width + 128)

    own_rows = lax.dynamic_slice_in_dim(table, first_slot, rep_dev, 0)
    own_rows = own_rows.astype(jnp.float32)
    mate_rows = jnp.dot(mate_rows_of, table, preferred_element_type=jnp.float32)

    def energy_of(rows):
        return rows[:, row_width] + (rows[:, row_width + 1] + rows[:, row_width + 2])

    own_energy = energy_of(own_rows)
    mate_energy = energy_of(mate_rows)
    swap_gain = beta_gap * (own_energy - mate_energy) * (1.0 / (64.0 * N * math.sqrt(N)))
    accept = swap_gain + noise > 0.0
    spins_out = jnp.where(
        accept[:, None], mate_rows[:, :row_width], own_rows[:, :row_width]
    )
    energies = jnp.where(accept, mate_energy, own_energy) * (1.0 / (N * math.sqrt(N)))
    return (spins_out.astype(jnp.bfloat16), energies)


def solution(mesh):
    fine = Mesh(mesh.devices.reshape(2, 2, 2, 16, 4), ("xh", "core", "xl", "z", "y"))
    rep, row, col = ("xh", "core"), ("xl", "z"), "y"
    in_specs = (
        P(rep, row),
        P(None, col, None, row),
        P(None, rep, row),
        P(row),
        P(),
        P(),
        P(),
    )
    out_specs = (P(rep, row), P(rep))
    return jax.shard_map(
        per_device, mesh=fine, in_specs=in_specs, out_specs=out_specs, check_vma=False
    )
```

```python
import math

import jax
import jax.numpy as jnp
from jax import lax
from jax.experimental import pallas as pl
from jax.experimental.pallas import tpu as pltpu
from jax.sharding import Mesh, PartitionSpec as P

N = 8192
SWEEPS = 10
NEVER = -3.0e38

GROUP = ("xh", "core")
PLANE = ("xl", "y")
LAYER = ("xh", "core", "xl", "y")


def sent_to_all(value, axes):
    length = lax.axis_size(axes)
    return lax.all_to_all(
        jnp.broadcast_to(value[None], (length, *value.shape)), axes, 0, 0, tiled=True
    )


def in_spin_order(gathered):
    n_core, n_xl, n_y, n_z, piece, width = gathered.shape
    shape = (n_z, n_core * n_y, piece, n_xl * width)

    def body(source, target, sems):
        copies = [
            pltpu.make_async_copy(
                source.at[core, xl, y],
                target.at[:, core * n_y + y, :, pl.ds(xl * width, width)],
                sems.at[core, xl, y],
            )
            for xl in range(n_xl)
            for core in range(n_core)
            for y in range(n_y)
        ]
        for copy in copies:
            copy.start()
        for copy in copies:
            copy.wait()

    ordered = pl.pallas_call(
        body,
        in_specs=[pl.BlockSpec(memory_space=pltpu.HBM)],
        out_specs=pl.BlockSpec(memory_space=pl.ANY),
        out_shape=jax.ShapeDtypeStruct(shape, gathered.dtype),
        scratch_shapes=[pltpu.SemaphoreType.DMA((n_core, n_xl, n_y))],
        compiler_params=pltpu.CompilerParams(vmem_limit_bytes=2 * 1024 * 1024),
        name="in_spin_order",
    )(pltpu.with_memory_space_constraint(gathered, pltpu.HBM))
    return ordered.reshape(-1, n_xl * width)


def left_lanes(shape):
    return lax.broadcasted_iota(jnp.int32, shape, len(shape) - 1) < shape[-1] // 2


def packed(value):
    half = value.shape[0] // 2
    return jnp.concatenate([value[:half], value[half:]], axis=1)


def first_terms(spins, blocks, core, xl, count):
    n_core, rows, width = blocks.shape
    half = spins.shape[0] // 2
    lanes = 2 * (n_core * rows // count)
    pairs = count // 2 // n_core

    def body(
        core_ref, xl_ref, spins_ref, blocks_ref, out_ref, one_ref, two_ref, spins_held, held_ref, sems
    ):
        spins_arrive = pltpu.make_async_copy(spins_ref, spins_held, sems.at[n_core + 2])
        arrive = [
            pltpu.make_async_copy(blocks_ref.at[n], held_ref.at[n], sems.at[n])
            for n in range(n_core)
        ]
        spins_arrive.start()
        for copy in arrive:
            copy.start()
        leave = [
            pltpu.make_async_copy(held_ref.at[core_ref[0]], one_ref, sems.at[n_core]),
            pltpu.make_async_copy(held_ref.at[1 - xl_ref[0]], two_ref, sems.at[n_core + 1]),
        ]
        spins_arrive.wait()
        is_left = left_lanes((half, lanes))
        for n in range(n_core):
            arrive[n].wait()
            if n == n_core - 1:
                for copy in leave:
                    copy.start()
            terms = lax.dot_general(
                spins_held[...],
                held_ref[n],
                (((1,), (1,)), ((), ())),
                preferred_element_type=jnp.float32,
            )
            for pair in range(pairs):
                both = terms[:, pair * lanes : (pair + 1) * lanes]
                top, bottom = both[:half], both[half:]
                even = jnp.where(is_left, top, pltpu.roll(bottom, lanes // 2, 1))
                odd = jnp.where(is_left, pltpu.roll(top, lanes // 2, 1), bottom)
                at = 2 * (n * pairs + pair)
                out_ref[at] = even.astype(jnp.bfloat16)
                out_ref[at + 1] = odd.astype(jnp.bfloat16)
        for copy in leave:
            copy.wait()

    return pl.pallas_call(
        body,
        in_specs=[
            pl.BlockSpec(memory_space=pltpu.SMEM),
            pl.BlockSpec(memory_space=pltpu.SMEM),
            pl.BlockSpec(memory_space=pl.ANY),
            pl.BlockSpec(memory_space=pl.ANY),
        ],
        out_specs=[pl.BlockSpec(memory_space=pltpu.VMEM)]
        + [pl.BlockSpec(memory_space=pl.ANY)] * 2,
        out_shape=[jax.ShapeDtypeStruct((count, half, lanes), jnp.bfloat16)]
        + [jax.ShapeDtypeStruct((rows, width), jnp.bfloat16)] * 2,
        scratch_shapes=[
            pltpu.VMEM(spins.shape, jnp.bfloat16),
            pltpu.VMEM((n_core, rows, width), jnp.bfloat16),
            pltpu.SemaphoreType.DMA((n_core + 3,)),
        ],
        compiler_params=pltpu.CompilerParams(vmem_limit_bytes=16 * 1024 * 1024),
        name="first_terms",
    )(
        core[None],
        xl[None],
        pltpu.with_memory_space_constraint(spins, pltpu.HBM),
        pltpu.with_memory_space_constraint(blocks, pltpu.HBM),
    )


def second_terms(rows, own_spins, blocks, own, far, parts):
    count, half, lanes = rows.shape
    depth, width = far.shape
    share = 2 * half // parts

    def body(own_ref, rows_ref, piece_ref, blocks_ref, far_ref, out_ref, all_ref, held_ref, sems):
        arrive = [
            pltpu.make_async_copy(blocks_ref.at[own_ref[0]], held_ref.at[0], sems.at[0]),
            pltpu.make_async_copy(far_ref, held_ref.at[1], sems.at[1]),
        ]
        for copy in arrive:
            copy.start()
        is_left = left_lanes((half, lanes))
        for pair in range(count // 2):
            even = rows_ref[2 * pair].astype(jnp.float32)
            odd = rows_ref[2 * pair + 1].astype(jnp.float32)
            top = jnp.where(is_left, even, pltpu.roll(odd, lanes // 2, 1))
            bottom = jnp.where(is_left, pltpu.roll(even, lanes // 2, 1), odd)
            at = pl.ds(pair * lanes, lanes)
            all_ref[0:half, at] = top.astype(jnp.bfloat16)
            all_ref[half : 2 * half, at] = bottom.astype(jnp.bfloat16)
        piece = piece_ref[...]
        beside = pl.ds(2 * width, lanes)
        out_ref[0 : parts // 2, :, beside] = piece.reshape(parts // 2, share, lanes)
        piece = pltpu.roll(piece, lanes // 2, 1)
        out_ref[parts // 2 : parts, :, beside] = piece.reshape(parts // 2, share, lanes)
        for n, copy in enumerate(arrive):
            copy.wait()
            terms = jnp.dot(all_ref[...], held_ref[n], preferred_element_type=jnp.float32)
            out_ref[:, :, n * width : (n + 1) * width] = terms.reshape(parts, share, width)

    return pl.pallas_call(
        body,
        out_shape=jax.ShapeDtypeStruct((parts, share, 2 * width + lanes), jnp.float32),
        in_specs=[
            pl.BlockSpec(memory_space=pltpu.SMEM),
            pl.BlockSpec(memory_space=pltpu.VMEM),
            pl.BlockSpec(memory_space=pltpu.VMEM),
            pl.BlockSpec(memory_space=pl.ANY),
            pl.BlockSpec(memory_space=pl.ANY),
        ],
        scratch_shapes=[
            pltpu.VMEM((2 * half, depth), jnp.bfloat16),
            pltpu.VMEM((2, depth, width), jnp.bfloat16),
            pltpu.SemaphoreType.DMA((2,)),
        ],
        compiler_params=pltpu.CompilerParams(vmem_limit_bytes=16 * 1024 * 1024),
        name="second_terms",
    )(own[None], rows, own_spins, pltpu.with_memory_space_constraint(blocks, pltpu.HBM), far)


def last_blocks(energy_rows, spins, group, sides, others):
    share, width = spins.shape
    part = width // sides
    lanes = energy_rows.shape[1]
    count = group * sides * others

    def body(rows_ref, spins_ref, out_ref):
        row = -0.5 * jnp.sum(rows_ref[...], axis=0, keepdims=True)
        lane = lax.broadcasted_iota(jnp.int32, (share, lanes), 1)
        sublane = lax.broadcasted_iota(jnp.int32, (share, lanes), 0)
        energy = jnp.sum(
            jnp.where(lane == sublane, jnp.broadcast_to(row, (share, lanes)), 0.0),
            axis=1,
            keepdims=True,
        )
        energy = jnp.broadcast_to(energy, (share, lanes))
        high = energy.astype(jnp.bfloat16).astype(jnp.float32)
        middle = (energy - high).astype(jnp.bfloat16).astype(jnp.float32)
        low = (energy - high) - middle
        terms = jnp.where(lane == 0, high, jnp.where(lane == 1, middle, low))
        terms = terms.astype(jnp.bfloat16)
        values = spins_ref[...].astype(jnp.bfloat16)
        for n in range(count):
            side = n // others % sides
            out_ref[n, :, 0:part] = values[:, side * part : (side + 1) * part]
            out_ref[n, :, part : part + lanes] = terms

    return pl.pallas_call(
        body,
        out_shape=jax.ShapeDtypeStruct((count, share, part + lanes), jnp.bfloat16),
        compiler_params=pltpu.CompilerParams(vmem_limit_bytes=8 * 1024 * 1024),
        name="last_blocks",
    )(energy_rows, spins)


def per_device(spin_init, couplings, flip_noise, colors, beta_steps, partners, swap_noise):
    rep_dev, row_width = spin_init.shape
    n_xl = lax.axis_size("xl")
    n_y = lax.axis_size("y")
    n_z = lax.axis_size("z")
    n_core = lax.axis_size("core")
    y_index = lax.axis_index("y")
    xl_index = lax.axis_index("xl")
    core_index = lax.axis_index("core")
    rep_index = lax.axis_index(GROUP)
    share = rep_dev // (n_xl * n_y)
    piece = row_width // n_y
    width = n_xl * row_width
    own_block = couplings.reshape(-1, row_width)

    first_slot = rep_index * rep_dev

    def metropolis(spins, fields, limit, scale):
        energy_cost = scale * (spins * fields)
        return jnp.where(energy_cost < limit, -spins, spins)

    blocks = own_block.reshape(n_core, -1, row_width)
    terms, core_half, cross = first_terms(
        spin_init, blocks, core_index, xl_index, n_xl * n_z
    )
    gathered = lax.all_gather(core_half, ("core", *PLANE))
    terms = lax.all_to_all(terms, ("xl", "z"), 0, 0, tiled=True)
    far = lax.ppermute(cross, ("xh", "xl"), [(0, 3), (3, 0), (1, 2), (2, 1)])
    all_betas = beta_steps.astype(jnp.float32)
    all_scales = all_betas * (1.0 / 16384.0)

    def scales(first, length):
        return lax.dynamic_slice_in_dim(all_scales, first, length)[:, None]

    slot_ids = first_slot + jnp.arange(rep_dev, dtype=jnp.int32)
    mate_ids = lax.dynamic_slice_in_dim(partners, first_slot, rep_dev)
    all_ids = jnp.arange(partners.shape[0], dtype=jnp.int32)[None, :]

    def picked(values, ids):
        return jnp.sum(jnp.where(ids[:, None] == all_ids, values[None, :], 0.0), axis=1)

    beta_gap = picked(all_betas, slot_ids) - picked(all_betas, mate_ids)
    noise = picked(swap_noise, jnp.minimum(slot_ids, mate_ids))
    mate_rows_of = (mate_ids[:, None] == all_ids).astype(jnp.bfloat16)

    def own_piece(value):
        return lax.dynamic_slice_in_dim(value, y_index * piece, piece, value.ndim - 1)

    limit = jnp.where(own_piece(colors)[None, :] == 0, own_piece(flip_noise[0]), NEVER)
    fields = terms.astype(jnp.float32).sum(axis=0)
    own_spins = packed(own_piece(spin_init)).astype(jnp.float32)
    own_scales = packed(jnp.broadcast_to(scales(first_slot, rep_dev), (rep_dev, piece)))
    own_spins = metropolis(own_spins, fields, packed(limit), own_scales)


    steps = jnp.arange(1, SWEEPS, dtype=jnp.int32)[:, None, None]

    def limits_of(xl):
        first = (xl * n_y + y_index) * share
        noise = lax.dynamic_slice_in_dim(flip_noise, first, share, 1)[1:]
        return jnp.where(colors[None, None, :] == steps % 2, noise, NEVER)

    is_left = xl_index == 0
    kept = limits_of(xl_index)
    other = limits_of(1 - xl_index)
    other = lax.ppermute(other, "xl", [(0, 1), (1, 0)])
    limits = jnp.concatenate(
        [jnp.where(is_left, kept, other), jnp.where(is_left, other, kept)], axis=2
    )
    limits = [limits[step] for step in range(SWEEPS - 1)]
    scale = scales(first_slot + lax.axis_index(PLANE) * share, share)

    own_spins, limits, scale, beta_gap, noise, mate_rows_of, far = lax.optimization_barrier(
        (own_spins, limits, scale, beta_gap, noise, mate_rows_of, far)
    )
    rows = sent_to_all(own_spins.astype(jnp.bfloat16), "z")
    partial = second_terms(rows, own_spins, blocks, xl_index, far, n_xl * n_y)
    partial = lax.all_to_all(partial, PLANE, 0, 0, tiled=True)
    fields = partial.reshape(n_xl, n_y, share, -1).sum(axis=1)
    fields = jnp.concatenate(
        [
            fields[side, :, :row_width] + fields[1 - side, :, row_width:width]
            for side in range(n_xl)
        ],
        axis=1,
    )
    spins = partial[:, :, width : width + piece]
    spins = spins.transpose(1, 0, 2).reshape(share, width)

    def layer_rows(spins):
        return sent_to_all(spins.astype(jnp.bfloat16), "z")

    def layer_fields(rows, layer_block):
        rows = rows.transpose(1, 0, 2).reshape(share, N)
        return jnp.dot(rows, layer_block, preferred_element_type=jnp.float32)

    spins = metropolis(spins, fields, limits[0], scale)
    spins = lax.optimization_barrier(spins)
    rows, gathered = lax.optimization_barrier((layer_rows(spins), gathered))
    layer_block = in_spin_order(
        gathered.reshape(n_core, n_xl, n_y, n_z, piece, row_width)
    )
    for limit in limits[1:]:
        spins = metropolis(spins, layer_fields(rows, layer_block), limit, scale)
        spins = lax.optimization_barrier(spins)
        rows = layer_rows(spins)

    layer_sum = jnp.sum(spins * layer_fields(rows, layer_block), axis=1)
    layer_sum = jnp.pad(layer_sum, (0, 128 - share))[None]
    energy_rows = sent_to_all(layer_sum, "z").reshape(n_z, 128)
    blocks = last_blocks(energy_rows, spins, lax.axis_size(GROUP), n_xl, n_y)
    table = lax.all_to_all(blocks, LAYER, 0, 0, tiled=True).reshape(-1, row_width + 128)

    own_rows = lax.dynamic_slice_in_dim(table, first_slot, rep_dev, 0)
    own_rows = own_rows.astype(jnp.float32)
    mate_rows = jnp.dot(mate_rows_of, table, preferred_element_type=jnp.float32)

    def energy_of(rows):
        return rows[:, row_width] + (rows[:, row_width + 1] + rows[:, row_width + 2])

    own_energy = energy_of(own_rows)
    mate_energy = energy_of(mate_rows)
    swap_gain = beta_gap * (own_energy - mate_energy) * (1.0 / (64.0 * N * math.sqrt(N)))
    accept = swap_gain + noise > 0.0
    spins_out = jnp.where(
        accept[:, None], mate_rows[:, :row_width], own_rows[:, :row_width]
    )
    energies = jnp.where(accept, mate_energy, own_energy) * (1.0 / (N * math.sqrt(N)))
    return (spins_out.astype(jnp.bfloat16), energies)


def solution(mesh):
    fine = Mesh(mesh.devices.reshape(2, 2, 2, 16, 4), ("xh", "core", "xl", "z", "y"))
    rep, row, col = ("xh", "core"), ("xl", "z"), "y"
    in_specs = (
        P(rep, row),
        P(None, col, None, row),
        P(None, rep, row),
        P(row),
        P(),
        P(),
        P(),
    )
    out_specs = (P(rep, row), P(rep))
    return jax.shard_map(
        per_device, mesh=fine, in_specs=in_specs, out_specs=out_specs, check_vma=False
    )
```

```python
import math

import jax
import jax.numpy as jnp
from jax import lax
from jax.experimental import pallas as pl
from jax.experimental.pallas import tpu as pltpu
from jax.sharding import Mesh, PartitionSpec as P

N = 8192
SWEEPS = 10
NEVER = -3.0e38

GROUP = ("xh", "core")
PLANE = ("xl", "y")
LAYER = ("xh", "core", "xl", "y")


def sent_to_all(value, axes):
    length = lax.axis_size(axes)
    return lax.all_to_all(
        jnp.broadcast_to(value[None], (length, *value.shape)), axes, 0, 0, tiled=True
    )


def in_spin_order(gathered):
    n_core, n_xl, n_y, n_z, piece, width = gathered.shape
    shape = (n_z, n_core * n_y, piece, n_xl * width)

    def body(source, target, sems):
        copies = [
            pltpu.make_async_copy(
                source.at[core, xl, y],
                target.at[:, core * n_y + y, :, pl.ds(xl * width, width)],
                sems.at[core, xl, y],
            )
            for xl in range(n_xl)
            for core in range(n_core)
            for y in range(n_y)
        ]
        for copy in copies:
            copy.start()
        for copy in copies:
            copy.wait()

    ordered = pl.pallas_call(
        body,
        in_specs=[pl.BlockSpec(memory_space=pltpu.HBM)],
        out_specs=pl.BlockSpec(memory_space=pl.ANY),
        out_shape=jax.ShapeDtypeStruct(shape, gathered.dtype),
        scratch_shapes=[pltpu.SemaphoreType.DMA((n_core, n_xl, n_y))],
        compiler_params=pltpu.CompilerParams(vmem_limit_bytes=2 * 1024 * 1024),
        name="in_spin_order",
    )(pltpu.with_memory_space_constraint(gathered, pltpu.HBM))
    return ordered.reshape(-1, n_xl * width)


def left_lanes(shape):
    return lax.broadcasted_iota(jnp.int32, shape, len(shape) - 1) < shape[-1] // 2


def packed(value):
    half = value.shape[0] // 2
    return jnp.concatenate([value[:half], value[half:]], axis=1)


def first_terms(spins, blocks, core, xl, count):
    n_core, rows, width = blocks.shape
    half = spins.shape[0] // 2
    lanes = 2 * (n_core * rows // count)
    pairs = count // 2 // n_core

    def body(
        core_ref, xl_ref, spins_ref, blocks_ref, out_ref, one_ref, two_ref, spins_held, held_ref, sems
    ):
        spins_arrive = pltpu.make_async_copy(spins_ref, spins_held, sems.at[n_core + 2])
        arrive = [
            pltpu.make_async_copy(blocks_ref.at[n], held_ref.at[n], sems.at[n])
            for n in range(n_core)
        ]
        spins_arrive.start()
        for copy in arrive:
            copy.start()
        leave = [
            pltpu.make_async_copy(held_ref.at[core_ref[0]], one_ref, sems.at[n_core]),
            pltpu.make_async_copy(held_ref.at[1 - xl_ref[0]], two_ref, sems.at[n_core + 1]),
        ]
        spins_arrive.wait()
        is_left = left_lanes((half, lanes))
        for n in range(n_core):
            arrive[n].wait()
            if n == n_core - 1:
                for copy in leave:
                    copy.start()
            terms = lax.dot_general(
                spins_held[...],
                held_ref[n],
                (((1,), (1,)), ((), ())),
                preferred_element_type=jnp.float32,
            )
            for pair in range(pairs):
                both = terms[:, pair * lanes : (pair + 1) * lanes]
                top, bottom = both[:half], both[half:]
                even = jnp.where(is_left, top, pltpu.roll(bottom, lanes // 2, 1))
                odd = jnp.where(is_left, pltpu.roll(top, lanes // 2, 1), bottom)
                at = 2 * (n * pairs + pair)
                out_ref[at] = even.astype(jnp.bfloat16)
                out_ref[at + 1] = odd.astype(jnp.bfloat16)
        for copy in leave:
            copy.wait()

    return pl.pallas_call(
        body,
        in_specs=[
            pl.BlockSpec(memory_space=pltpu.SMEM),
            pl.BlockSpec(memory_space=pltpu.SMEM),
            pl.BlockSpec(memory_space=pl.ANY),
            pl.BlockSpec(memory_space=pl.ANY),
        ],
        out_specs=[pl.BlockSpec(memory_space=pltpu.VMEM)]
        + [pl.BlockSpec(memory_space=pl.ANY)] * 2,
        out_shape=[jax.ShapeDtypeStruct((count, half, lanes), jnp.bfloat16)]
        + [jax.ShapeDtypeStruct((rows, width), jnp.bfloat16)] * 2,
        scratch_shapes=[
            pltpu.VMEM(spins.shape, jnp.bfloat16),
            pltpu.VMEM((n_core, rows, width), jnp.bfloat16),
            pltpu.SemaphoreType.DMA((n_core + 3,)),
        ],
        compiler_params=pltpu.CompilerParams(vmem_limit_bytes=16 * 1024 * 1024),
        name="first_terms",
    )(
        core[None],
        xl[None],
        pltpu.with_memory_space_constraint(spins, pltpu.HBM),
        pltpu.with_memory_space_constraint(blocks, pltpu.HBM),
    )


def second_terms(rows, own_spins, blocks, own, far, parts):
    count, half, lanes = rows.shape
    depth, width = far.shape
    share = 2 * half // parts

    def body(own_ref, rows_ref, piece_ref, blocks_ref, far_ref, out_ref, all_ref, held_ref, sems):
        arrive = [
            pltpu.make_async_copy(blocks_ref.at[own_ref[0]], held_ref.at[0], sems.at[0]),
            pltpu.make_async_copy(far_ref, held_ref.at[1], sems.at[1]),
        ]
        for copy in arrive:
            copy.start()
        is_left = left_lanes((half, lanes))
        for pair in range(count // 2):
            even = rows_ref[2 * pair].astype(jnp.float32)
            odd = rows_ref[2 * pair + 1].astype(jnp.float32)
            top = jnp.where(is_left, even, pltpu.roll(odd, lanes // 2, 1))
            bottom = jnp.where(is_left, pltpu.roll(even, lanes // 2, 1), odd)
            at = pl.ds(pair * lanes, lanes)
            all_ref[0:half, at] = top.astype(jnp.bfloat16)
            all_ref[half : 2 * half, at] = bottom.astype(jnp.bfloat16)
        piece = piece_ref[...]
        beside = pl.ds(2 * width, lanes)
        out_ref[0 : parts // 2, :, beside] = piece.reshape(parts // 2, share, lanes)
        piece = pltpu.roll(piece, lanes // 2, 1)
        out_ref[parts // 2 : parts, :, beside] = piece.reshape(parts // 2, share, lanes)
        for n, copy in enumerate(arrive):
            copy.wait()
            terms = jnp.dot(all_ref[...], held_ref[n], preferred_element_type=jnp.float32)
            out_ref[:, :, n * width : (n + 1) * width] = terms.reshape(parts, share, width)

    return pl.pallas_call(
        body,
        out_shape=jax.ShapeDtypeStruct((parts, share, 2 * width + lanes), jnp.float32),
        in_specs=[
            pl.BlockSpec(memory_space=pltpu.SMEM),
            pl.BlockSpec(memory_space=pltpu.VMEM),
            pl.BlockSpec(memory_space=pltpu.VMEM),
            pl.BlockSpec(memory_space=pl.ANY),
            pl.BlockSpec(memory_space=pl.ANY),
        ],
        scratch_shapes=[
            pltpu.VMEM((2 * half, depth), jnp.bfloat16),
            pltpu.VMEM((2, depth, width), jnp.bfloat16),
            pltpu.SemaphoreType.DMA((2,)),
        ],
        compiler_params=pltpu.CompilerParams(vmem_limit_bytes=16 * 1024 * 1024),
        name="second_terms",
    )(own[None], rows, own_spins, pltpu.with_memory_space_constraint(blocks, pltpu.HBM), far)


def last_blocks(energy_rows, spins, group, sides, others):
    share, width = spins.shape
    part = width // sides
    lanes = energy_rows.shape[1]
    count = group * sides * others

    def body(rows_ref, spins_ref, out_ref):
        row = -0.5 * jnp.sum(rows_ref[...], axis=0, keepdims=True)
        lane = lax.broadcasted_iota(jnp.int32, (share, lanes), 1)
        sublane = lax.broadcasted_iota(jnp.int32, (share, lanes), 0)
        energy = jnp.sum(
            jnp.where(lane == sublane, jnp.broadcast_to(row, (share, lanes)), 0.0),
            axis=1,
            keepdims=True,
        )
        energy = jnp.broadcast_to(energy, (share, lanes))
        high = energy.astype(jnp.bfloat16).astype(jnp.float32)
        middle = (energy - high).astype(jnp.bfloat16).astype(jnp.float32)
        low = (energy - high) - middle
        terms = jnp.where(lane == 0, high, jnp.where(lane == 1, middle, low))
        terms = terms.astype(jnp.bfloat16)
        values = spins_ref[...].astype(jnp.bfloat16)
        for n in range(count):
            side = n // others % sides
            out_ref[n, :, 0:part] = values[:, side * part : (side + 1) * part]
            out_ref[n, :, part : part + lanes] = terms

    return pl.pallas_call(
        body,
        out_shape=jax.ShapeDtypeStruct((count, share, part + lanes), jnp.bfloat16),
        compiler_params=pltpu.CompilerParams(vmem_limit_bytes=8 * 1024 * 1024),
        name="last_blocks",
    )(energy_rows, spins)


def per_device(spin_init, couplings, flip_noise, colors, beta_steps, partners, swap_noise):
    rep_dev, row_width = spin_init.shape
    n_xl = lax.axis_size("xl")
    n_y = lax.axis_size("y")
    n_z = lax.axis_size("z")
    n_core = lax.axis_size("core")
    y_index = lax.axis_index("y")
    xl_index = lax.axis_index("xl")
    core_index = lax.axis_index("core")
    rep_index = lax.axis_index(GROUP)
    share = rep_dev // (n_xl * n_y)
    piece = row_width // n_y
    width = n_xl * row_width
    own_block = couplings.reshape(-1, row_width)

    first_slot = rep_index * rep_dev

    def metropolis(spins, fields, limit, scale):
        energy_cost = scale * (spins * fields)
        return jnp.where(energy_cost < limit, -spins, spins)

    blocks = own_block.reshape(n_core, -1, row_width)
    terms, core_half, cross = first_terms(
        spin_init, blocks, core_index, xl_index, n_xl * n_z
    )
    gathered = lax.all_gather(core_half, ("core", *PLANE))
    terms = lax.all_to_all(terms, ("xl", "z"), 0, 0, tiled=True)
    far = lax.ppermute(cross, ("xh", "xl"), [(0, 3), (3, 0), (1, 2), (2, 1)])
    all_betas = beta_steps.astype(jnp.float32)
    all_scales = all_betas * (1.0 / 16384.0)

    def scales(first, length):
        return lax.dynamic_slice_in_dim(all_scales, first, length)[:, None]

    slot_ids = first_slot + jnp.arange(rep_dev, dtype=jnp.int32)
    mate_ids = lax.dynamic_slice_in_dim(partners, first_slot, rep_dev)
    all_ids = jnp.arange(partners.shape[0], dtype=jnp.int32)[None, :]

    def picked(values, ids):
        return jnp.sum(jnp.where(ids[:, None] == all_ids, values[None, :], 0.0), axis=1)

    beta_gap = picked(all_betas, slot_ids) - picked(all_betas, mate_ids)
    noise = picked(swap_noise, jnp.minimum(slot_ids, mate_ids))
    mate_rows_of = (mate_ids[:, None] == all_ids).astype(jnp.bfloat16)

    def own_piece(value):
        return lax.dynamic_slice_in_dim(value, y_index * piece, piece, value.ndim - 1)

    limit = jnp.where(own_piece(colors)[None, :] == 0, own_piece(flip_noise[0]), NEVER)
    fields = terms.astype(jnp.float32).sum(axis=0)
    own_spins = packed(own_piece(spin_init)).astype(jnp.float32)
    own_scales = packed(jnp.broadcast_to(scales(first_slot, rep_dev), (rep_dev, piece)))
    own_spins = metropolis(own_spins, fields, packed(limit), own_scales)


    steps = jnp.arange(1, SWEEPS, dtype=jnp.int32)[:, None, None]

    def limits_of(xl):
        first = (xl * n_y + y_index) * share
        noise = lax.dynamic_slice_in_dim(flip_noise, first, share, 1)[1:]
        return jnp.where(colors[None, None, :] == steps % 2, noise, NEVER)

    is_left = xl_index == 0
    kept = limits_of(xl_index)
    other = limits_of(1 - xl_index)
    other = lax.ppermute(other, "xl", [(0, 1), (1, 0)])
    limits = jnp.concatenate(
        [jnp.where(is_left, kept, other), jnp.where(is_left, other, kept)], axis=2
    )
    limits = [limits[step] for step in range(SWEEPS - 1)]
    scale = scales(first_slot + lax.axis_index(PLANE) * share, share)

    rows = sent_to_all(own_spins.astype(jnp.bfloat16), "z")
    partial = second_terms(rows, own_spins, blocks, xl_index, far, n_xl * n_y)
    partial, limits, scale, beta_gap, noise, mate_rows_of = lax.optimization_barrier(
        (partial, limits, scale, beta_gap, noise, mate_rows_of)
    )
    partial = lax.all_to_all(partial.astype(jnp.int16), PLANE, 0, 0, tiled=True)
    partial = partial.astype(jnp.float32)
    fields = partial.reshape(n_xl, n_y, share, -1).sum(axis=1)
    fields = jnp.concatenate(
        [
            fields[side, :, :row_width] + fields[1 - side, :, row_width:width]
            for side in range(n_xl)
        ],
        axis=1,
    )
    spins = partial[:, :, width : width + piece]
    spins = spins.transpose(1, 0, 2).reshape(share, width)

    def layer_rows(spins):
        return sent_to_all(spins.astype(jnp.bfloat16), "z")

    def layer_fields(rows, layer_block):
        rows = rows.transpose(1, 0, 2).reshape(share, N)
        return jnp.dot(rows, layer_block, preferred_element_type=jnp.float32)

    spins = metropolis(spins, fields, limits[0], scale)
    spins = lax.optimization_barrier(spins)
    rows, gathered = lax.optimization_barrier((layer_rows(spins), gathered))
    layer_block = in_spin_order(
        gathered.reshape(n_core, n_xl, n_y, n_z, piece, row_width)
    )
    for limit in limits[1:]:
        spins = metropolis(spins, layer_fields(rows, layer_block), limit, scale)
        spins = lax.optimization_barrier(spins)
        rows = layer_rows(spins)

    layer_sum = jnp.sum(spins * layer_fields(rows, layer_block), axis=1)
    layer_sum = jnp.pad(layer_sum, (0, 128 - share))[None]
    energy_rows = sent_to_all(layer_sum, "z").reshape(n_z, 128)
    blocks = last_blocks(energy_rows, spins, lax.axis_size(GROUP), n_xl, n_y)
    table = lax.all_to_all(blocks, LAYER, 0, 0, tiled=True).reshape(-1, row_width + 128)

    own_rows = lax.dynamic_slice_in_dim(table, first_slot, rep_dev, 0)
    own_rows = own_rows.astype(jnp.float32)
    mate_rows = jnp.dot(mate_rows_of, table, preferred_element_type=jnp.float32)

    def energy_of(rows):
        return rows[:, row_width] + (rows[:, row_width + 1] + rows[:, row_width + 2])

    own_energy = energy_of(own_rows)
    mate_energy = energy_of(mate_rows)
    swap_gain = beta_gap * (own_energy - mate_energy) * (1.0 / (64.0 * N * math.sqrt(N)))
    accept = swap_gain + noise > 0.0
    spins_out = jnp.where(
        accept[:, None], mate_rows[:, :row_width], own_rows[:, :row_width]
    )
    energies = jnp.where(accept, mate_energy, own_energy) * (1.0 / (N * math.sqrt(N)))
    return (spins_out.astype(jnp.bfloat16), energies)


def solution(mesh):
    fine = Mesh(mesh.devices.reshape(2, 2, 2, 16, 4), ("xh", "core", "xl", "z", "y"))
    rep, row, col = ("xh", "core"), ("xl", "z"), "y"
    in_specs = (
        P(rep, row),
        P(None, col, None, row),
        P(None, rep, row),
        P(row),
        P(),
        P(),
        P(),
    )
    out_specs = (P(rep, row), P(rep))
    return jax.shard_map(
        per_device, mesh=fine, in_specs=in_specs, out_specs=out_specs, check_vma=False
    )
```

```python
import math

import jax
import jax.numpy as jnp
from jax import lax
from jax.experimental import pallas as pl
from jax.experimental.pallas import tpu as pltpu
from jax.sharding import Mesh, PartitionSpec as P

N = 8192
SWEEPS = 10
NEVER = -3.0e38

GROUP = ("xh", "core")
PLANE = ("xl", "y")
LAYER = ("xh", "core", "xl", "y")


def sent_to_all(value, axes):
    length = lax.axis_size(axes)
    return lax.all_to_all(
        jnp.broadcast_to(value[None], (length, *value.shape)), axes, 0, 0, tiled=True
    )


def in_spin_order(gathered, rows):
    n_core, n_xl, n_y, n_z, piece, width = gathered.shape
    shape = (n_z, n_core * n_y, piece, n_xl * width)
    depth = n_core * n_y * piece
    groups = 2
    each = n_z // groups
    share = rows.shape[1]

    def body(source, rows_ref, target, fields_ref, sems):
        copies = [
            [
                pltpu.make_async_copy(
                    source.at[core, xl, y, pl.ds(group * each, each)],
                    target.at[
                        pl.ds(group * each, each), core * n_y + y, :, pl.ds(xl * width, width)
                    ],
                    sems.at[group, core, xl, y],
                )
                for xl in range(n_xl)
                for core in range(n_core)
                for y in range(n_y)
            ]
            for group in range(groups)
        ]
        for group in copies:
            for copy in group:
                copy.start()
        fields = jnp.zeros((share, n_xl * width), jnp.float32)
        for n, group in enumerate(copies):
            for copy in group:
                copy.wait()
            for z in range(n * each, (n + 1) * each):
                block = target[z].reshape(depth, n_xl * width)
                fields += jnp.dot(rows_ref[z], block, preferred_element_type=jnp.float32)
        fields_ref[...] = fields

    ordered, fields = pl.pallas_call(
        body,
        in_specs=[
            pl.BlockSpec(memory_space=pltpu.HBM),
            pl.BlockSpec(memory_space=pltpu.VMEM),
        ],
        out_specs=[pl.BlockSpec(memory_space=pltpu.VMEM)] * 2,
        out_shape=[
            pltpu.VMEM(shape, gathered.dtype),
            jax.ShapeDtypeStruct((share, n_xl * width), jnp.float32),
        ],
        scratch_shapes=[pltpu.SemaphoreType.DMA((groups, n_core, n_xl, n_y))],
        compiler_params=pltpu.CompilerParams(vmem_limit_bytes=2 * 1024 * 1024),
        name="in_spin_order",
    )(pltpu.with_memory_space_constraint(gathered, pltpu.HBM), rows)
    return ordered.reshape(-1, n_xl * width), fields


def left_lanes(shape):
    return lax.broadcasted_iota(jnp.int32, shape, len(shape) - 1) < shape[-1] // 2


def packed(value):
    half = value.shape[0] // 2
    return jnp.concatenate([value[:half], value[half:]], axis=1)


def first_terms(spins, blocks, core, xl, count):
    n_core, rows, width = blocks.shape
    half = spins.shape[0] // 2
    lanes = 2 * (n_core * rows // count)
    pairs = count // 2 // n_core

    def body(
        core_ref, xl_ref, spins_ref, blocks_ref, out_ref, one_ref, two_ref, spins_held, held_ref, sems
    ):
        spins_arrive = pltpu.make_async_copy(spins_ref, spins_held, sems.at[n_core + 2])
        arrive = [
            pltpu.make_async_copy(blocks_ref.at[n], held_ref.at[n], sems.at[n])
            for n in range(n_core)
        ]
        spins_arrive.start()
        for copy in arrive:
            copy.start()
        leave = [
            pltpu.make_async_copy(held_ref.at[core_ref[0]], one_ref, sems.at[n_core]),
            pltpu.make_async_copy(held_ref.at[1 - xl_ref[0]], two_ref, sems.at[n_core + 1]),
        ]
        spins_arrive.wait()
        is_left = left_lanes((half, lanes))
        for n in range(n_core):
            arrive[n].wait()
            if n == n_core - 1:
                for copy in leave:
                    copy.start()
            terms = lax.dot_general(
                spins_held[...],
                held_ref[n],
                (((1,), (1,)), ((), ())),
                preferred_element_type=jnp.float32,
            )
            for pair in range(pairs):
                both = terms[:, pair * lanes : (pair + 1) * lanes]
                top, bottom = both[:half], both[half:]
                even = jnp.where(is_left, top, pltpu.roll(bottom, lanes // 2, 1))
                odd = jnp.where(is_left, pltpu.roll(top, lanes // 2, 1), bottom)
                at = 2 * (n * pairs + pair)
                out_ref[at] = even.astype(jnp.bfloat16)
                out_ref[at + 1] = odd.astype(jnp.bfloat16)
        for copy in leave:
            copy.wait()

    return pl.pallas_call(
        body,
        in_specs=[
            pl.BlockSpec(memory_space=pltpu.SMEM),
            pl.BlockSpec(memory_space=pltpu.SMEM),
            pl.BlockSpec(memory_space=pl.ANY),
            pl.BlockSpec(memory_space=pl.ANY),
        ],
        out_specs=[pl.BlockSpec(memory_space=pltpu.VMEM)]
        + [pl.BlockSpec(memory_space=pl.ANY)] * 2,
        out_shape=[jax.ShapeDtypeStruct((count, half, lanes), jnp.bfloat16)]
        + [jax.ShapeDtypeStruct((rows, width), jnp.bfloat16)] * 2,
        scratch_shapes=[
            pltpu.VMEM(spins.shape, jnp.bfloat16),
            pltpu.VMEM((n_core, rows, width), jnp.bfloat16),
            pltpu.SemaphoreType.DMA((n_core + 3,)),
        ],
        compiler_params=pltpu.CompilerParams(vmem_limit_bytes=16 * 1024 * 1024),
        name="first_terms",
    )(
        core[None],
        xl[None],
        pltpu.with_memory_space_constraint(spins, pltpu.HBM),
        pltpu.with_memory_space_constraint(blocks, pltpu.HBM),
    )


def second_terms(rows, own_spins, blocks, own, far, parts):
    count, half, lanes = rows.shape
    depth, width = far.shape
    share = 2 * half // parts

    def body(own_ref, rows_ref, piece_ref, blocks_ref, far_ref, out_ref, all_ref, held_ref, sems):
        arrive = [
            pltpu.make_async_copy(blocks_ref.at[own_ref[0]], held_ref.at[0], sems.at[0]),
            pltpu.make_async_copy(far_ref, held_ref.at[1], sems.at[1]),
        ]
        for copy in arrive:
            copy.start()
        is_left = left_lanes((half, lanes))
        for pair in range(count // 2):
            even = rows_ref[2 * pair].astype(jnp.float32)
            odd = rows_ref[2 * pair + 1].astype(jnp.float32)
            top = jnp.where(is_left, even, pltpu.roll(odd, lanes // 2, 1))
            bottom = jnp.where(is_left, pltpu.roll(even, lanes // 2, 1), odd)
            at = pl.ds(pair * lanes, lanes)
            all_ref[0:half, at] = top.astype(jnp.bfloat16)
            all_ref[half : 2 * half, at] = bottom.astype(jnp.bfloat16)
        piece = piece_ref[...]
        beside = pl.ds(2 * width, lanes)
        out_ref[0 : parts // 2, :, beside] = piece.reshape(parts // 2, share, lanes)
        piece = pltpu.roll(piece, lanes // 2, 1)
        out_ref[parts // 2 : parts, :, beside] = piece.reshape(parts // 2, share, lanes)
        for n, copy in enumerate(arrive):
            copy.wait()
            terms = jnp.dot(all_ref[...], held_ref[n], preferred_element_type=jnp.float32)
            out_ref[:, :, n * width : (n + 1) * width] = terms.reshape(parts, share, width)

    return pl.pallas_call(
        body,
        out_shape=jax.ShapeDtypeStruct((parts, share, 2 * width + lanes), jnp.float32),
        in_specs=[
            pl.BlockSpec(memory_space=pltpu.SMEM),
            pl.BlockSpec(memory_space=pltpu.VMEM),
            pl.BlockSpec(memory_space=pltpu.VMEM),
            pl.BlockSpec(memory_space=pl.ANY),
            pl.BlockSpec(memory_space=pl.ANY),
        ],
        scratch_shapes=[
            pltpu.VMEM((2 * half, depth), jnp.bfloat16),
            pltpu.VMEM((2, depth, width), jnp.bfloat16),
            pltpu.SemaphoreType.DMA((2,)),
        ],
        compiler_params=pltpu.CompilerParams(vmem_limit_bytes=16 * 1024 * 1024),
        name="second_terms",
    )(own[None], rows, own_spins, pltpu.with_memory_space_constraint(blocks, pltpu.HBM), far)


def last_blocks(energy_rows, spins, group, sides, others):
    share, width = spins.shape
    part = width // sides
    lanes = energy_rows.shape[1]
    count = group * sides * others

    def body(rows_ref, spins_ref, out_ref):
        row = -0.5 * jnp.sum(rows_ref[...], axis=0, keepdims=True)
        lane = lax.broadcasted_iota(jnp.int32, (share, lanes), 1)
        sublane = lax.broadcasted_iota(jnp.int32, (share, lanes), 0)
        energy = jnp.sum(
            jnp.where(lane == sublane, jnp.broadcast_to(row, (share, lanes)), 0.0),
            axis=1,
            keepdims=True,
        )
        energy = jnp.broadcast_to(energy, (share, lanes))
        high = energy.astype(jnp.bfloat16).astype(jnp.float32)
        middle = (energy - high).astype(jnp.bfloat16).astype(jnp.float32)
        low = (energy - high) - middle
        terms = jnp.where(lane == 0, high, jnp.where(lane == 1, middle, low))
        terms = terms.astype(jnp.bfloat16)
        values = spins_ref[...].astype(jnp.bfloat16)
        for n in range(count):
            side = n // others % sides
            out_ref[n, :, 0:part] = values[:, side * part : (side + 1) * part]
            out_ref[n, :, part : part + lanes] = terms

    return pl.pallas_call(
        body,
        out_shape=jax.ShapeDtypeStruct((count, share, part + lanes), jnp.bfloat16),
        compiler_params=pltpu.CompilerParams(vmem_limit_bytes=8 * 1024 * 1024),
        name="last_blocks",
    )(energy_rows, spins)


def per_device(spin_init, couplings, flip_noise, colors, beta_steps, partners, swap_noise):
    rep_dev, row_width = spin_init.shape
    n_xl = lax.axis_size("xl")
    n_y = lax.axis_size("y")
    n_z = lax.axis_size("z")
    n_core = lax.axis_size("core")
    y_index = lax.axis_index("y")
    xl_index = lax.axis_index("xl")
    core_index = lax.axis_index("core")
    rep_index = lax.axis_index(GROUP)
    share = rep_dev // (n_xl * n_y)
    piece = row_width // n_y
    width = n_xl * row_width
    own_block = couplings.reshape(-1, row_width)

    first_slot = rep_index * rep_dev

    def metropolis(spins, fields, limit, scale):
        energy_cost = scale * (spins * fields)
        return jnp.where(energy_cost < limit, -spins, spins)

    blocks = own_block.reshape(n_core, -1, row_width)
    terms, core_half, cross = first_terms(
        spin_init, blocks, core_index, xl_index, n_xl * n_z
    )
    gathered = lax.all_gather(core_half, ("core", *PLANE))
    terms = lax.all_to_all(terms, ("xl", "z"), 0, 0, tiled=True)
    far = lax.ppermute(cross, ("xh", "xl"), [(0, 3), (3, 0), (1, 2), (2, 1)])
    all_betas = beta_steps.astype(jnp.float32)
    all_scales = all_betas * (1.0 / 16384.0)

    def scales(first, length):
        return lax.dynamic_slice_in_dim(all_scales, first, length)[:, None]

    slot_ids = first_slot + jnp.arange(rep_dev, dtype=jnp.int32)
    mate_ids = lax.dynamic_slice_in_dim(partners, first_slot, rep_dev)
    all_ids = jnp.arange(partners.shape[0], dtype=jnp.int32)[None, :]

    def picked(values, ids):
        return jnp.sum(jnp.where(ids[:, None] == all_ids, values[None, :], 0.0), axis=1)

    beta_gap = picked(all_betas, slot_ids) - picked(all_betas, mate_ids)
    noise = picked(swap_noise, jnp.minimum(slot_ids, mate_ids))
    mate_rows_of = (mate_ids[:, None] == all_ids).astype(jnp.bfloat16)

    def own_piece(value):
        return lax.dynamic_slice_in_dim(value, y_index * piece, piece, value.ndim - 1)

    limit = jnp.where(own_piece(colors)[None, :] == 0, own_piece(flip_noise[0]), NEVER)
    fields = terms.astype(jnp.float32).sum(axis=0)
    own_spins = packed(own_piece(spin_init)).astype(jnp.float32)
    own_scales = packed(jnp.broadcast_to(scales(first_slot, rep_dev), (rep_dev, piece)))
    own_spins = metropolis(own_spins, fields, packed(limit), own_scales)


    steps = jnp.arange(1, SWEEPS, dtype=jnp.int32)[:, None, None]

    def limits_of(xl):
        first = (xl * n_y + y_index) * share
        noise = lax.dynamic_slice_in_dim(flip_noise, first, share, 1)[1:]
        return jnp.where(colors[None, None, :] == steps % 2, noise, NEVER)

    is_left = xl_index == 0
    kept = limits_of(xl_index)
    other = limits_of(1 - xl_index)
    other = lax.ppermute(other, "xl", [(0, 1), (1, 0)])
    limits = jnp.concatenate(
        [jnp.where(is_left, kept, other), jnp.where(is_left, other, kept)], axis=2
    )
    limits = [limits[step] for step in range(SWEEPS - 1)]
    scale = scales(first_slot + lax.axis_index(PLANE) * share, share)

    rows = sent_to_all(own_spins.astype(jnp.bfloat16), "z")
    partial = second_terms(rows, own_spins, blocks, xl_index, far, n_xl * n_y)
    partial, limits, scale, beta_gap, noise, mate_rows_of = lax.optimization_barrier(
        (partial, limits, scale, beta_gap, noise, mate_rows_of)
    )
    partial = lax.all_to_all(partial.astype(jnp.int16), PLANE, 0, 0, tiled=True)
    partial = partial.astype(jnp.float32)
    fields = partial.reshape(n_xl, n_y, share, -1).sum(axis=1)
    fields = jnp.concatenate(
        [
            fields[side, :, :row_width] + fields[1 - side, :, row_width:width]
            for side in range(n_xl)
        ],
        axis=1,
    )
    spins = partial[:, :, width : width + piece]
    spins = spins.transpose(1, 0, 2).reshape(share, width)

    def layer_rows(spins):
        return sent_to_all(spins.astype(jnp.bfloat16), "z")

    def layer_fields(rows, layer_block):
        rows = rows.transpose(1, 0, 2).reshape(share, N)
        return jnp.dot(rows, layer_block, preferred_element_type=jnp.float32)

    spins = metropolis(spins, fields, limits[0], scale)
    spins = lax.optimization_barrier(spins)
    rows, gathered = lax.optimization_barrier((layer_rows(spins), gathered))
    layer_block, fields = in_spin_order(
        gathered.reshape(n_core, n_xl, n_y, n_z, piece, row_width), rows
    )
    for limit in limits[1:]:
        spins = metropolis(spins, fields, limit, scale)
        spins = lax.optimization_barrier(spins)
        fields = layer_fields(layer_rows(spins), layer_block)

    layer_sum = jnp.sum(spins * fields, axis=1)
    layer_sum = jnp.pad(layer_sum, (0, 128 - share))[None]
    energy_rows = sent_to_all(layer_sum, "z").reshape(n_z, 128)
    blocks = last_blocks(energy_rows, spins, lax.axis_size(GROUP), n_xl, n_y)
    table = lax.all_to_all(blocks, LAYER, 0, 0, tiled=True).reshape(-1, row_width + 128)

    own_rows = lax.dynamic_slice_in_dim(table, first_slot, rep_dev, 0)
    own_rows = own_rows.astype(jnp.float32)
    mate_rows = jnp.dot(mate_rows_of, table, preferred_element_type=jnp.float32)

    def energy_of(rows):
        return rows[:, row_width] + (rows[:, row_width + 1] + rows[:, row_width + 2])

    own_energy = energy_of(own_rows)
    mate_energy = energy_of(mate_rows)
    swap_gain = beta_gap * (own_energy - mate_energy) * (1.0 / (64.0 * N * math.sqrt(N)))
    accept = swap_gain + noise > 0.0
    spins_out = jnp.where(
        accept[:, None], mate_rows[:, :row_width], own_rows[:, :row_width]
    )
    energies = jnp.where(accept, mate_energy, own_energy) * (1.0 / (N * math.sqrt(N)))
    return (spins_out.astype(jnp.bfloat16), energies)


def solution(mesh):
    fine = Mesh(mesh.devices.reshape(2, 2, 2, 16, 4), ("xh", "core", "xl", "z", "y"))
    rep, row, col = ("xh", "core"), ("xl", "z"), "y"
    in_specs = (
        P(rep, row),
        P(None, col, None, row),
        P(None, rep, row),
        P(row),
        P(),
        P(),
        P(),
    )
    out_specs = (P(rep, row), P(rep))
    return jax.shard_map(
        per_device, mesh=fine, in_specs=in_specs, out_specs=out_specs, check_vma=False
    )
```
